256 devices in a mesh: gx: 8 (over z), gy: 4 (over x_lo, core), gz: 8 (over y, x_hi).
Axes of the slice: x: 4 (x_hi: 2, x_lo: 2; x = x_hi * 2 + x_lo), y: 4, z: 8, core: 2. Of those that a mesh axis runs over, the one named last changes fastest.
Arguments:
- source: float32 [128, 128, 512], P('gx', 'gz', 'gy'), may hold values from -0.6 to 0.6
- shift: float32 [1], replicated, may hold values from 1e-05 to 0.0001
Outputs:
- solution: float32 [128, 128, 512], P('gx', 'gz', 'gy')
The draws below stay inside these ranges and needn't reach their ends.
All inputs are finite; a program needn't handle non-finite values.
Results may differ from the reference program's by a relative error of at most 0.0004.
Values sent between devices are 32-bit elements; how exact they have to be, the bound alone decides.
A program may use at most 64 MiB of HBM per device.

```python
import math
import jax
import jax.numpy as jnp
from jax import lax

LEVELS = 4
NU_PRE = 1
NU_POST = 1
N0 = 128
N1 = 128
N2 = 512


MEAN_LEVEL = 1e-06


def draw_source(key, part):
    rough_key = jax.random.fold_in(jax.random.fold_in(key, 11), 0)
    rough = jnp.clip(0.1 * jax.random.normal(rough_key, (N0, N1, N2), jnp.float32), -0.59, 0.59)
    return rough - jnp.mean(rough) + MEAN_LEVEL


def setup_inputs(seed: int = 0) -> dict:
    streams_of = jax.random.split(jax.random.key(seed), 3)
    source = draw_source(jax.random.fold_in(streams_of[2], 71), 0)
    shift = jnp.clip(jnp.exp(jax.random.uniform(streams_of[1], (1,), jnp.float32, math.log(9.999999747378752e-06), math.log(0.0001))), 9.999999747378752e-06, 0.0001)
    return {"source": source, "shift": shift}


DAMPING = 6.0 / 7.0
PRECISE = lax.Precision.HIGHEST
CUBIC_EVEN = (-5.0 / 128.0, 35.0 / 128.0, 105.0 / 128.0, -7.0 / 128.0)
CUBIC_ODD = (-7.0 / 128.0, 105.0 / 128.0, 35.0 / 128.0, -5.0 / 128.0)
LINEAR_EVEN = (0.25, 0.75)
LINEAR_ODD = (0.75, 0.25)


def wrapped(values, width):
    return jnp.pad(values, width, mode="wrap")


def neighbours(padded):
    center = padded[1:-1, 1:-1, 1:-1]
    beside_all = padded[2:, 1:-1, 1:-1] + padded[:-2, 1:-1, 1:-1]
    beside_all = beside_all + padded[1:-1, 2:, 1:-1] + padded[1:-1, :-2, 1:-1]
    beside_all = beside_all + padded[1:-1, 1:-1, 2:] + padded[1:-1, 1:-1, :-2]
    return center, beside_all


def defect(padded, forcing, weight_nb, diagonal):
    center, beside_all = neighbours(padded)
    return forcing - (diagonal * center - weight_nb * beside_all)


def relaxed(padded, forcing, weight_nb, diagonal):
    center, beside_all = neighbours(padded)
    return center + DAMPING * (forcing - (diagonal * center - weight_nb * beside_all)) / diagonal


def coarsen(values):
    values = values[0::2] + values[1::2]
    values = values[:, 0::2] + values[:, 1::2]
    values = values[:, :, 0::2] + values[:, :, 1::2]
    return 0.125 * values


def refine_axis(padded, dimension, even_weights, odd_weights):
    margin = len(even_weights) // 2
    length = padded.shape[dimension] - 2 * margin
    even_cells = even_weights[0] * lax.slice_in_dim(padded, 0, length, axis=dimension)
    odd_cells = odd_weights[0] * lax.slice_in_dim(padded, 1, 1 + length, axis=dimension)
    for offset in range(1, len(even_weights)):
        even_cells = even_cells + even_weights[offset] * lax.slice_in_dim(padded, offset, offset + length, axis=dimension)
        odd_cells = odd_cells + odd_weights[offset] * lax.slice_in_dim(padded, offset + 1, offset + 1 + length, axis=dimension)
    stacked = jnp.stack([even_cells, odd_cells], axis=dimension + 1)
    new_shape = list(even_cells.shape)
    new_shape[dimension] = 2 * length
    return stacked.reshape(new_shape)


def refine(padded, even_weights, odd_weights):
    for dimension in range(3):
        padded = refine_axis(padded, dimension, even_weights, odd_weights)
    return padded


def tables(cells_count):
    indices = jnp.arange(cells_count, dtype=jnp.int32)
    angles = ((indices[:, None] * indices[None, :]) % cells_count).astype(jnp.float32) * (2.0 * math.pi / cells_count)
    return jnp.cos(angles), jnp.sin(angles)


def along_axis(matrix, values, dimension):
    product = jnp.tensordot(matrix, values, axes=([1], [dimension]), precision=PRECISE)
    return jnp.moveaxis(product, 0, dimension)


def coarse_solve(forcing, shift_value, weight_nb):
    cosine_table, sine_table = tables(forcing.shape[0])
    real_part = along_axis(cosine_table, forcing, 0)
    imag_part = -along_axis(sine_table, forcing, 0)
    for dimension in (1, 2):
        cosine_table, sine_table = tables(forcing.shape[dimension])
        real_next = along_axis(cosine_table, real_part, dimension) + along_axis(sine_table, imag_part, dimension)
        imag_part = along_axis(cosine_table, imag_part, dimension) - along_axis(sine_table, real_part, dimension)
        real_part = real_next
    cosines = [jnp.cos(jnp.arange(cells_count, dtype=jnp.float32) * (2.0 * math.pi / cells_count)) for cells_count in forcing.shape]
    eigenvalue = weight_nb * (6.0 - 2.0 * cosines[0][:, None, None] - 2.0 * cosines[1][None, :, None] - 2.0 * cosines[2][None, None, :]) + shift_value
    real_part = real_part / eigenvalue
    imag_part = imag_part / eigenvalue
    for dimension in (0, 1):
        cosine_table, sine_table = tables(forcing.shape[dimension])
        real_next = along_axis(cosine_table, real_part, dimension) - along_axis(sine_table, imag_part, dimension)
        imag_part = along_axis(cosine_table, imag_part, dimension) + along_axis(sine_table, real_part, dimension)
        real_part = real_next
    cosine_table, sine_table = tables(forcing.shape[2])
    real_part = along_axis(cosine_table, real_part, 2) - along_axis(sine_table, imag_part, 2)
    return real_part / float(forcing.size)


def vcycle(grid_level, iterate, forcing, shift_value):
    weight_nb = 0.25 ** grid_level
    diagonal = 6.0 * weight_nb + shift_value
    for sweep_index in range(NU_PRE):
        iterate = relaxed(wrapped(iterate, 1), forcing, weight_nb, diagonal)
    residue = coarsen(defect(wrapped(iterate, 1), forcing, weight_nb, diagonal))
    if grid_level + 1 == LEVELS - 1:
        correction = coarse_solve(residue, shift_value, 0.25 ** (grid_level + 1))
    else:
        correction = vcycle(grid_level + 1, jnp.zeros_like(residue), residue, shift_value)
    iterate = iterate + refine(wrapped(correction, 1), LINEAR_EVEN, LINEAR_ODD)
    for sweep_index in range(NU_POST):
        iterate = relaxed(wrapped(iterate, 1), forcing, weight_nb, diagonal)
    return iterate


def reference(source, shift):
    shift_value = shift[0]
    sources = [source]
    for grid_level in range(1, LEVELS):
        sources.append(coarsen(sources[-1]))
    iterate = coarse_solve(sources[-1], shift_value, 0.25 ** (LEVELS - 1))
    for grid_level in range(LEVELS - 2, -1, -1):
        iterate = refine(wrapped(iterate, 2), CUBIC_EVEN, CUBIC_ODD)
        iterate = vcycle(grid_level, iterate, sources[grid_level], shift_value)
    return iterate
```

```python
import functools
import math

import jax
import jax.numpy as jnp
import ml_dtypes
import numpy as np
from jax import lax
from jax.experimental import pallas as pl
from jax.experimental.pallas import tpu as pltpu
from jax.sharding import PartitionSpec as P

MESH = pl.DeviceIdType.MESH
DAMPING = 6.0 / 7.0
LINEAR = ({-1: 0.25, 0: 0.75}, {0: 0.75, 1: 0.25})
CUBIC = (
    {-2: -5.0 / 128, -1: 35.0 / 128, 0: 105.0 / 128, 1: -7.0 / 128},
    {-1: -7.0 / 128, 0: 105.0 / 128, 1: 35.0 / 128, 2: -5.0 / 128},
)
GX, GY, GZ = 8, 4, 8
N_GATHER = 7 + 15 + 16
N_SEMS = 3 * N_GATHER + 4 + 24


(RZ1, RZ2, RH, QZ21, PZ21, QZ10M, QZ10H, PZ10M, PZ10H, WZ, WZL, WQ, WQL, WP, WPL) = range(15)


def fourier(n):
    j = np.arange(n)
    rows, eig = [np.full(n, math.sqrt(1.0 / n))], [0.0]
    for k in range(1, n // 2):
        for f in (np.cos, np.sin):
            rows.append(math.sqrt(2.0 / n) * f(2 * np.pi * ((k * j) % n) / n))
            eig.append(2 - 2 * np.cos(2 * np.pi * k / n))
    rows.append(math.sqrt(1.0 / n) * np.where(j % 2, -1.0, 1.0))
    eig.append(4.0)
    return np.array(rows), np.array(eig)


def halves(m):
    high = m.astype(ml_dtypes.bfloat16)
    return high, (m - high.astype(np.float64)).astype(ml_dtypes.bfloat16)


def tables():
    m = np.zeros((15, 128, 128))
    for i in range(64):
        for p in range(2):
            m[RZ1, 2 * i + p, 8 + i] = 0.125
    for i in range(32):
        for p in range(2):
            m[RZ2, 8 + 2 * i + p, i::32] = 0.125
    for k in range(4):
        for p in range(2):
            m[RH, 2 * k + p, 72 + k] = 0.125
            m[RH, 120 + 2 * k + p, 4 + k] = 0.125
    for z in range(-8, 72):
        i, p = divmod(z, 2)
        for t, w in ((QZ21, CUBIC[p]), (PZ21, LINEAR[p])):
            for off, weight in w.items():
                m[t, (32 + i + off) % 128, 8 + z] += weight
    for z in range(-8, 136):
        i, p = divmod(z, 2)
        own = 0 <= z < 128
        for t, w in ((QZ10M if own else QZ10H, CUBIC[p]), (PZ10M if own else PZ10H, LINEAR[p])):
            for off, weight in w.items():
                m[t, 8 + i + off, z % 128] += weight
    hz, ez = fourier(64)
    down = np.zeros((128, 64))
    for z in range(128):
        down[z, z // 2] = 0.125
    m[WZ, :, :64] = down @ hz.T
    for t, weights in ((WQ, CUBIC), (WP, LINEAR)):
        up = np.zeros((64, 128))
        for z in range(128):
            i, p = divmod(z, 2)
            for off, weight in weights[p].items():
                up[(i + off) % 64, z] += weight
        m[t, :64, :] = hz @ up
    mats = m.astype(ml_dtypes.bfloat16)
    for t in (WZ, WQ, WP):
        mats[t], mats[t + 1] = halves(m[t])
    h, e = fourier(16)
    hxy = np.zeros((256, 256))
    for r in range(256):
        jp, x, g = r // 128, (r // 8) % 16, r % 8
        hxy[:, r] = np.kron(h[:, x], h[:, 2 * g + jp])
    both = np.stack([*halves(hxy), *halves(hxy.T)])
    lam = np.ones((256, 128))
    lam[:, :64] = 0.25**3 * ((e[:, None] + e[None, :]).reshape(256, 1) + ez[None, :])
    return mats, both, lam.astype(np.float32)


def dot(a, b):
    return jnp.dot(a, b, preferred_element_type=jnp.float32)


def split(x):
    high = x.astype(jnp.bfloat16)
    return high, (x - high.astype(jnp.float32)).astype(jnp.bfloat16)


def mm2(x, w):
    high, low = split(x)
    return dot(high, w) + dot(low, w)


def mm3(x, w, w_low):
    high, low = split(x)
    return dot(high, w) + dot(low, w) + dot(high, w_low)


def left3(w, w_low, x):
    high, low = split(x)
    return dot(w, high) + dot(w, low) + dot(w_low, high)


def roll(x, shift, axis):
    shift %= x.shape[axis]
    return x if shift == 0 else pltpu.roll(x, shift, axis)


def weighted(weights, at):
    total = None
    for off, weight in weights.items():
        term = weight * at(off)
        total = term if total is None else total + term
    return total


def loop(start, stop, body):
    def step(i, carry):
        body(i)
        return carry

    lax.fori_loop(start, stop, step, 0)


def lanes(shape):
    return lax.broadcasted_iota(jnp.int32, shape, len(shape) - 1)


def kernel(
    shift_ref, src, mats_hbm, hxy_hbm, lam_hbm, out,
    mats, hxy, lam, A, W, f1o, LR1, LR0, H0, F1, F0M, F0H,
    G2, U2, V2, T3, TZ2, B1, V1, U1, T1, tmp, TZM, TZH, BM, BH, VM, VH, TM, TH, RM, RHH, R1, D1, E1,
    csem, ss, rs,
):
    gx, gy, gz = lax.axis_index("gx"), lax.axis_index("gy"), lax.axis_index("gz")
    core = lax.rem(gy, 2)

    def peer(dx, dy, dz):
        return (lax.rem(gx + dx % GX, GX), lax.rem(gy + dy % GY, GY), lax.rem(gz + dz % GZ, GZ))

    partner = (gx, gy + 1 - 2 * core, gz)

    loads = [
        pltpu.make_async_copy(mats_hbm, mats, csem.at[0]),
        pltpu.make_async_copy(hxy_hbm, hxy, csem.at[1]),
        pltpu.make_async_copy(lam_hbm, lam, csem.at[2]),
    ]
    for load in loads:
        load.start()

    barrier = pltpu.get_barrier_semaphore()
    friends = [(d, 0, 0) for d in range(1, 8)]
    friends += [(0, a, b) for a in (0, 2) for b in range(8) if (a, b) != (0, 0)]
    friends += [(0, 1, 0), (0, 3, 0)]
    friends += [(a, 0, b) for a in (1, 7) for b in (1, 7)]
    for f in friends:
        pl.semaphore_signal(barrier, inc=1, device_id=peer(*f), device_id_type=MESH)

    used = [0]

    def remote(source, target, device):
        k = used[0]
        used[0] += 1
        return pltpu.make_async_remote_copy(
            src_ref=source, dst_ref=target, send_sem=ss.at[k], recv_sem=rs.at[k],
            device_id=device, device_id_type=MESH,
        )

    shift = shift_ref[0]
    w = [0.25**k for k in range(4)]
    d = [6.0 * w[k] + shift for k in range(3)]
    c = [jnp.max(DAMPING / jnp.full((8, 128), d[k], jnp.float32)) for k in range(3)]

    def wrap(u):
        for j in range(4):
            u[j, 0] = u[j, 32]
            u[j, 33] = u[j, 1]

    def beside2(u, i, n):
        mid = [u[j, pl.ds(i + 1, n)] for j in range(4)]
        sums = []
        for j in range(4):
            s = u[j, pl.ds(i + 2, n)] + u[j, pl.ds(i, n)]
            s = s + (mid[j + 1] if j < 3 else roll(mid[0], -1, 1))
            s = s + (mid[j - 1] if j > 0 else roll(mid[3], 1, 1))
            s = s + roll(mid[j], -1, 2) + roll(mid[j], 1, 2)
            sums.append(s)
        return mid, sums

    def sweep2(u, v):
        def body(t):
            i = 4 * t
            mid, sums = beside2(u, i, 4)
            for j in range(4):
                g = G2[j, pl.ds(i, 4)]
                v[j, pl.ds(i + 1, 4)] = mid[j] + c[2] * (g - (d[2] * mid[j] - w[2] * sums[j]))

        loop(0, 8, body)
        wrap(v)

    def keep3(values, t):
        for jp in range(2):
            s = values[2 * jp] + values[2 * jp + 1]
            T3[jp, 2 * t] = s[0] + s[1]
            T3[jp, 2 * t + 1] = s[2] + s[3]

    def defect2(v):
        def body(t):
            i = 4 * t
            mid, sums = beside2(v, i, 4)
            keep3([G2[j, pl.ds(i, 4)] - (d[2] * mid[j] - w[2] * sums[j]) for j in range(4)], t)

        loop(0, 8, body)

    def solve3(t, weights):
        x = T3[...].reshape(256, 128)
        x = mm3(x, mats[WZ], mats[WZL])
        x = left3(hxy[0], hxy[1], x)
        x = x / (lam[...] + shift)
        x = left3(hxy[2], hxy[3], x)
        x = mm3(x, mats[t], mats[t + 1]).reshape(2, 16, 8, 128)
        result = []
        for j in range(4):
            jp, p = divmod(j, 2)

            def y_at(off):
                s, k = divmod(jp + off, 2)
                return roll(x[k], -s, 1)

            rows = weighted(weights[p], y_at)

            def x_at(off):
                return jnp.concatenate([rows[off % 16 :], rows[: off % 16]], axis=0) if off else rows

            pair = [weighted(weights[q], x_at) for q in range(2)]
            result.append(jnp.stack(pair, axis=1).reshape(32, 8, 128))
        return result

    def correct2():
        e = solve3(WP, LINEAR)
        for j in range(4):
            V2[j, 1:33] = V2[j, 1:33] + e[j]
        wrap(V2)
        sweep2(V2, U2)

    def cycle2_zero():
        def body(t):
            for j in range(4):
                V2[j, pl.ds(4 * t + 1, 4)] = c[2] * G2[j, pl.ds(4 * t, 4)]

        loop(0, 8, body)
        wrap(V2)
        defect2(V2)
        correct2()

    def restrict12(source, row):
        for x in range(4):
            s = None
            for a in range(2):
                for b in range(2):
                    part = source[2 * x + a, pl.ds(row + b, 4, stride=2), :]
                    s = part if s is None else s + part
            tmp[4 * x : 4 * x + 4] = s
        z = mm2(tmp[...], mats[RZ2])
        row_of = lax.broadcasted_iota(jnp.int32, (16, 128), 0)
        z = jnp.where(lax.div(lanes((16, 128)), 32) == lax.rem(row_of, 4), z, 0.0)
        z = z + roll(z, -1, 0)
        tmp[...] = z + roll(z, -2, 0)

    def gather_first(k):
        A[k, 8:12] = tmp[pl.ds(0, 4, stride=4), :]
        copies = []
        for dx in (4, 3, 5, 2, 6, 1, 7):
            slot = (2 - dx) % 8
            copies.append(remote(A.at[k, pl.ds(8, 4)], A.at[k, pl.ds(4 * slot, 4)], peer(dx, 0, 0)))
        for copy in copies:
            copy.start()
        return copies

    far = {0: 0, 1: 1, 2: 1, 3: 2, 4: 2, 5: 2, 6: 1, 7: 1}
    order = [(a, b) for a in (0, 2) for b in range(8) if (a, b) != (0, 0)]

    def gather_second(k, first):
        for copy in first:
            copy.wait_recv()
        W[k, 1, 32:64] = A[k]
        copies = {}
        for a, b in order:
            copies[a, b] = remote(
                A.at[k], W.at[k, (1 - a) % 4, pl.ds(32 * ((1 - b) % 8), 32)], peer(0, a, b)
            )
        for a, b in sorted(order, key=lambda o: -far[o[1]]):
            copies[a, b].start()
        return copies

    def gather_third(k, second):
        relays = []

        def relay(a, b):
            g, s = (1 - a) % 4, pl.ds(32 * ((1 - b) % 8), 32)
            to = lax.rem(g + 3 + 2 * core, 4)
            relays.append(remote(W.at[k, g, s], W.at[k, to, s], partner))
            relays[-1].start()

        relay(0, 0)
        for a, b in sorted(order, key=lambda o: far[o[1]]):
            second[a, b].wait_recv()
            relay(a, b)
        for copy in relays:
            copy.wait_recv()
        return relays

    def unpack(k):
        group = lax.div(lanes((8, 128)), 32)

        def body(x):
            blocks = [W[k, g, pl.ds(x, 8, stride=32), :] for g in range(4)]
            for j in range(4):
                total = roll(blocks[0], -32 * j, 1)
                for g in range(1, 4):
                    total = jnp.where(group == g, roll(blocks[g], 32 * (g - j), 1), total)
                G2[j, x] = total

        loop(0, 32, body)

    def refine21(table, weights):
        x = U2[:, 3:19].reshape(512, 128)
        TZ2[...] = mm2(x, mats[table]).reshape(4, 16, 8, 128)

        def body(t):
            for p in range(2):
                planes = [weighted(weights[p], lambda off: TZ2[j, t + 2 + off]) for j in range(4)]
                for j in range(4):
                    for q in range(2):

                        def y_at(off):
                            s, k = divmod(j + off, 4)
                            return roll(planes[k], -s, 0)

                        B1[2 * t + p, pl.ds(2 * j + q, 8, stride=8), :] = weighted(weights[q], y_at)

        loop(0, 12, body)

    def beside1(get, i):
        mid = get(i)
        s = get(i + 1) + get(i - 1)
        s = s + roll(mid, -1, 0) + roll(mid, 1, 0)
        s = s + roll(mid, -1, 1) + roll(mid, 1, 1)
        return mid, s

    def defect_of(mid, s, f, k):
        return f - (d[k] * mid - w[k] * s)

    def beside0(i):
        lane = lanes((32, 128))
        mid = [VM[i], VH[i]]
        up = [roll(m, -1, 1) for m in mid]
        down = [roll(m, 1, 1) for m in mid]
        sums = []
        for k, ref in enumerate((VM, VH)):
            s = ref[i + 1] + ref[i - 1]
            s = s + roll(mid[k], -1, 0) + roll(mid[k], 1, 0)
            s = s + jnp.where(lane == 127, up[1 - k], up[k]) + jnp.where(lane == 0, down[1 - k], down[k])
            sums.append(s)
        return mid, sums

    loads[0].wait()
    rows = []
    for x in range(8):
        s = None
        for a in range(2):
            for b in range(2):
                part = src[2 * x + a, pl.ds(b, 8, stride=2), :]
                s = part if s is None else s + part
        rows.append(s)
    f1o[...] = mm2(jnp.concatenate(rows, axis=0), mats[RZ1]).reshape(8, 8, 128)
    restrict12(f1o, 0)
    pl.semaphore_wait(barrier, len(friends))
    pending = []
    first = gather_first(0)
    pending += first
    side = []
    for dy, k in ((1, 0), (3, 1)):
        side.append(remote(f1o, LR1.at[k], peer(0, dy, 0)))
    for dy, k in ((1, 0), (3, 1)):
        side.append(remote(src, LR0.at[k], peer(0, dy, 0)))
    for copy in side:
        copy.start()
    pending += side

    second = gather_second(0, first)
    pending += second.values()

    side[0].wait_recv()
    side[1].wait_recv()
    lane = lanes((8, 8, 128))
    F1[8:16, 8:16] = jnp.where(
        lane < 8,
        roll(LR1[0], 64, 2),
        jnp.where(lane < 72, f1o[...], jnp.where(lane < 80, roll(LR1[1], 64, 2), 0.0)),
    )
    corner1 = []
    around = [(1, 0), (-1, 0), (0, 1), (0, -1), (1, 1), (1, -1), (-1, 1), (-1, -1)]
    for dx, dz in around:
        corner1.append(
            remote(
                F1.at[pl.ds(8, 8), pl.ds(8, 8)],
                F1.at[pl.ds(8 - 8 * dx, 8), pl.ds(8 - 8 * dz, 8)],
                peer(dx, 0, dz),
            )
        )
    for copy in corner1:
        copy.start()
    pending += corner1

    side[2].wait_recv()
    side[3].wait_recv()

    def halo0(i):
        lane = lanes((16, 128))
        H0[i] = jnp.where(lane < 8, LR0[1, i], jnp.where(lane >= 120, LR0[0, i], 0.0))
        F0M[i + 6, 8:24] = src[i]
        F0H[i + 6, 8:24] = H0[i]

    loop(0, 16, halo0)

    third = gather_third(0, second)
    pending += third

    corner0 = []
    for dx, dz in around:
        n_x, from_x, to_x = {0: (16, 0, 6), 1: (6, 10, 0), -1: (6, 0, 22)}[dx]
        n_y, from_y, to_y = {0: (16, 0, 8), 1: (8, 8, 0), -1: (8, 0, 24)}[dz]
        for source, target in ((src, F0M), (H0, F0H)):
            corner0.append(
                remote(
                    source.at[pl.ds(from_x, n_x), pl.ds(from_y, n_y)],
                    target.at[pl.ds(to_x, n_x), pl.ds(to_y, n_y)],
                    peer(dx, 0, dz),
                )
            )
    for copy in corner0:
        copy.start()
    pending += corner0

    unpack(0)
    loads[1].wait()
    loads[2].wait()

    def sum3(t):
        keep3([G2[j, pl.ds(4 * t, 4)] for j in range(4)], t)

    loop(0, 8, sum3)
    u = solve3(WQ, CUBIC)
    for j in range(4):
        U2[j, 1:33] = u[j]
    wrap(U2)
    sweep2(U2, V2)
    defect2(V2)
    correct2()

    refine21(QZ21, CUBIC)
    for copy in corner1:
        copy.wait_recv()

    def pre1(i):
        mid, s = beside1(lambda k: B1[k, 0:24], i)
        V1[i] = mid + c[1] * defect_of(mid, s, F1[i], 1)

    loop(1, 23, pre1)

    def res1(i):
        mid, s = beside1(lambda k: V1[k], i)
        T1[i - 8] = defect_of(mid, s, F1[i], 1)

    loop(8, 16, res1)
    restrict12(T1, 8)
    first = gather_first(1)
    second = gather_second(1, first)
    third = gather_third(1, second)
    pending += first + list(second.values()) + third
    unpack(1)
    cycle2_zero()
    refine21(PZ21, LINEAR)

    def add1(i):
        V1[i] = V1[i] + B1[i, 0:24]

    loop(2, 22, add1)

    def post1(i):
        mid, s = beside1(lambda k: V1[k], i)
        U1[i - 3] = mid + c[1] * defect_of(mid, s, F1[i], 1)

    loop(3, 21, post1)

    u = U1[...].reshape(432, 128)
    TZM[...] = mm2(u, mats[QZ10M]).reshape(18, 24, 128)
    TZH[...] = mm2(u, mats[QZ10H]).reshape(18, 24, 128)

    def cubic0(t):
        for source, target in ((TZM, BM), (TZH, BH)):
            for p in range(2):
                plane = weighted(CUBIC[p], lambda off: source[t + 2 + off])
                at = {off: roll(plane, -(4 + off), 0)[0:16] for off in range(-2, 3)}
                for q in range(2):
                    target[2 * t + p, pl.ds(q, 16, stride=2), :] = weighted(CUBIC[q], at.__getitem__)

    loop(0, 14, cubic0)
    for copy in corner0:
        copy.wait_recv()

    def pre0(i):
        lane = lanes((32, 128))
        refs = (BM, BH)
        mid = [ref[i] for ref in refs]
        up = [roll(m, -1, 1) for m in mid]
        down = [roll(m, 1, 1) for m in mid]
        for k, (f, v) in enumerate(((F0M, VM), (F0H, VH))):
            s = refs[k][i + 1] + refs[k][i - 1]
            s = s + roll(mid[k], -1, 0) + roll(mid[k], 1, 0)
            s = s + jnp.where(lane == 127, up[1 - k], up[k]) + jnp.where(lane == 0, down[1 - k], down[k])
            v[i] = mid[k] + c[0] * defect_of(mid[k], s, f[i], 0)

    loop(1, 27, pre0)

    def res0(t):
        for a in range(2):
            i = 2 * t + 2 + a
            mid, sums = beside0(i)
            for k, (f, target) in enumerate(((F0M, TM), (F0H, TH))):
                r = defect_of(mid[k], sums[k], f[i], 0)
                target[t] = r if a == 0 else target[t] + r
        for source, target in ((TM, RM), (TH, RHH)):
            target[t] = source[t, pl.ds(0, 16, stride=2), :] + source[t, pl.ds(1, 16, stride=2), :]

    loop(0, 12, res0)
    R1[...] = (
        mm2(RM[...].reshape(192, 128), mats[RZ1]) + mm2(RHH[...].reshape(192, 128), mats[RH])
    ).reshape(12, 16, 128)

    def zero1(i):
        D1[i] = c[1] * R1[i]

    loop(0, 12, zero1)

    def res1b(i):
        mid, s = beside1(lambda k: D1[k], i)
        T1[i - 2, 0:16] = defect_of(mid, s, R1[i], 1)

    loop(2, 10, res1b)
    restrict12(T1, 4)
    first = gather_first(2)
    second = gather_second(2, first)
    third = gather_third(2, second)
    pending += first + list(second.values()) + third
    unpack(2)
    cycle2_zero()
    refine21(PZ21, LINEAR)

    def add1b(i):
        D1[i] = D1[i] + B1[i + 6, 4:20]

    loop(0, 12, add1b)
    E1[0] = jnp.zeros((16, 128), jnp.float32)
    E1[11] = jnp.zeros((16, 128), jnp.float32)

    def post1b(i):
        mid, s = beside1(lambda k: D1[k], i)
        E1[i] = mid + c[1] * defect_of(mid, s, R1[i], 1)

    loop(1, 11, post1b)

    e = E1[...].reshape(192, 128)
    TZM[0:12, 0:16] = mm2(e, mats[PZ10M]).reshape(12, 16, 128)
    TZH[0:12, 0:16] = mm2(e, mats[PZ10H]).reshape(12, 16, 128)

    def linear0(t):
        for source, target, v in ((TZM, BM, VM), (TZH, BH, VH)):
            for p in range(2):
                plane = weighted(LINEAR[p], lambda off: source[t + 1 + off, 0:16])
                i = 2 * t + 4 + p
                for q in range(2):
                    target[i, pl.ds(q, 16, stride=2), :] = weighted(LINEAR[q], lambda off: roll(plane, -off, 0))
                v[i] = v[i] + target[i]

    loop(0, 10, linear0)

    def post0(i):
        mid, sums = beside0(i)
        v = mid[0] + c[0] * defect_of(mid[0], sums[0], F0M[i], 0)
        out[i - 6] = v[8:24]

    loop(6, 22, post0)
    for copy in pending:
        copy.wait_send()


def solution(mesh):
    mats, hxy, lam = tables()
    f32 = jnp.float32
    vmem = pltpu.VMEM
    scratch = [
        vmem((15, 128, 128), jnp.bfloat16),
        vmem((4, 256, 256), jnp.bfloat16),
        vmem((256, 128), f32),
        vmem((3, 32, 128), f32),
        vmem((3, 4, 256, 128), f32),
        vmem((8, 8, 128), f32),
        vmem((2, 8, 8, 128), f32),
        vmem((2, 16, 16, 128), f32),
        vmem((16, 16, 128), f32),
        vmem((24, 24, 128), f32),
        vmem((28, 32, 128), f32),
        vmem((28, 32, 128), f32),
        vmem((4, 32, 8, 128), f32),
        vmem((4, 34, 8, 128), f32),
        vmem((4, 34, 8, 128), f32),
        vmem((2, 16, 8, 128), f32),
        vmem((4, 16, 8, 128), f32),
        vmem((24, 64, 128), f32),
        vmem((24, 24, 128), f32),
        vmem((18, 24, 128), f32),
        vmem((8, 24, 128), f32),
        vmem((16, 128), f32),
        vmem((18, 24, 128), f32),
        vmem((18, 24, 128), f32),
        vmem((28, 32, 128), f32),
        vmem((28, 32, 128), f32),
        vmem((28, 32, 128), f32),
        vmem((28, 32, 128), f32),
        vmem((12, 32, 128), f32),
        vmem((12, 32, 128), f32),
        vmem((12, 16, 128), f32),
        vmem((12, 16, 128), f32),
        vmem((12, 16, 128), f32),
        vmem((12, 16, 128), f32),
        vmem((12, 16, 128), f32),
        pltpu.SemaphoreType.DMA((3,)),
        pltpu.SemaphoreType.DMA((N_SEMS,)),
        pltpu.SemaphoreType.DMA((N_SEMS,)),
    ]

    def step(source, shift):
        return pl.pallas_call(
            kernel,
            out_shape=jax.ShapeDtypeStruct(source.shape, f32),
            in_specs=[
                pl.BlockSpec(memory_space=pltpu.SMEM),
                pl.BlockSpec(memory_space=vmem),
                pl.BlockSpec(memory_space=pl.ANY),
                pl.BlockSpec(memory_space=pl.ANY),
                pl.BlockSpec(memory_space=pl.ANY),
            ],
            out_specs=pl.BlockSpec(memory_space=vmem),
            scratch_shapes=scratch,
            compiler_params=pltpu.CompilerParams(collective_id=0, has_side_effects=True),
            name="fcycle",
        )(shift, source, jnp.asarray(mats), jnp.asarray(hxy), jnp.asarray(lam))

    spec = P("gx", "gz", "gy")
    return jax.shard_map(step, mesh=mesh, in_specs=(spec, P()), out_specs=spec, check_vma=False)
```

```python
import functools
import math

import jax
import jax.numpy as jnp
import ml_dtypes
import numpy as np
from jax import lax
from jax.experimental import pallas as pl
from jax.experimental.pallas import tpu as pltpu
from jax.sharding import PartitionSpec as P

MESH = pl.DeviceIdType.MESH
DAMPING = 6.0 / 7.0
LINEAR = ({-1: 0.25, 0: 0.75}, {0: 0.75, 1: 0.25})
CUBIC = (
    {-2: -5.0 / 128, -1: 35.0 / 128, 0: 105.0 / 128, 1: -7.0 / 128},
    {-1: -7.0 / 128, 0: 105.0 / 128, 1: 35.0 / 128, 2: -5.0 / 128},
)
GX, GY, GZ = 8, 4, 8
N_GATHER = 7 + 15 + 16
N_SEMS = 3 * N_GATHER + 4 + 24
SLOT = 33


(RZ1, RZ2, RH, QZ21, PZ21, QZ10M, QZ10H, PZ10M, PZ10H, WZ, WZL, WQ, WQL, WP, WPL) = range(15)


def fourier(n):
    j = np.arange(n)
    rows, eig = [np.full(n, math.sqrt(1.0 / n))], [0.0]
    for k in range(1, n // 2):
        for f in (np.cos, np.sin):
            rows.append(math.sqrt(2.0 / n) * f(2 * np.pi * ((k * j) % n) / n))
            eig.append(2 - 2 * np.cos(2 * np.pi * k / n))
    rows.append(math.sqrt(1.0 / n) * np.where(j % 2, -1.0, 1.0))
    eig.append(4.0)
    return np.array(rows), np.array(eig)


def halves(m):
    high = m.astype(ml_dtypes.bfloat16)
    return high, (m - high.astype(np.float64)).astype(ml_dtypes.bfloat16)


def tables():
    m = np.zeros((15, 128, 128))
    for i in range(64):
        for p in range(2):
            m[RZ1, 2 * i + p, 8 + i] = 0.125
    for i in range(32):
        for p in range(2):
            m[RZ2, 8 + 2 * i + p, i::32] = 0.125
    for k in range(4):
        for p in range(2):
            m[RH, 2 * k + p, 72 + k] = 0.125
            m[RH, 120 + 2 * k + p, 4 + k] = 0.125
    for z in range(-8, 72):
        i, p = divmod(z, 2)
        for t, w in ((QZ21, CUBIC[p]), (PZ21, LINEAR[p])):
            for off, weight in w.items():
                m[t, (32 + i + off) % 128, 8 + z] += weight
    for z in range(-8, 136):
        i, p = divmod(z, 2)
        own = 0 <= z < 128
        for t, w in ((QZ10M if own else QZ10H, CUBIC[p]), (PZ10M if own else PZ10H, LINEAR[p])):
            for off, weight in w.items():
                m[t, 8 + i + off, z % 128] += weight
    hz, ez = fourier(64)
    down = np.zeros((128, 64))
    for z in range(128):
        down[z, z // 2] = 0.125
    m[WZ, :, :64] = down @ hz.T
    for t, weights in ((WQ, CUBIC), (WP, LINEAR)):
        up = np.zeros((64, 128))
        for z in range(128):
            i, p = divmod(z, 2)
            for off, weight in weights[p].items():
                up[(i + off) % 64, z] += weight
        m[t, :64, :] = hz @ up
    mats = m.astype(ml_dtypes.bfloat16)
    for t in (WZ, WQ, WP):
        mats[t], mats[t + 1] = halves(m[t])
    h, e = fourier(16)
    hxy = np.zeros((256, 256))
    for r in range(256):
        jp, x, g = r // 128, (r // 8) % 16, r % 8
        hxy[:, r] = np.kron(h[:, x], h[:, 2 * g + jp])
    both = np.stack([*halves(hxy), *halves(hxy.T)])
    lam = np.ones((256, 128))
    lam[:, :64] = 0.25**3 * ((e[:, None] + e[None, :]).reshape(256, 1) + ez[None, :])
    return mats, both, lam.astype(np.float32)


def dot(a, b):
    return jnp.dot(a, b, preferred_element_type=jnp.float32)


def split(x):
    high = x.astype(jnp.bfloat16)
    return high, (x - high.astype(jnp.float32)).astype(jnp.bfloat16)


def mm2(x, w):
    high, low = split(x)
    return dot(high, w) + dot(low, w)


def mm3(x, w, w_low):
    high, low = split(x)
    return dot(high, w) + dot(low, w) + dot(high, w_low)


def left3(w, w_low, x):
    high, low = split(x)
    return dot(w, high) + dot(w, low) + dot(w_low, high)


def roll(x, shift, axis):
    shift %= x.shape[axis]
    return x if shift == 0 else pltpu.roll(x, shift, axis)


def weighted(weights, at):
    total = None
    for off, weight in weights.items():
        term = weight * at(off)
        total = term if total is None else total + term
    return total


def loop(start, stop, body, unroll=1):
    trips = (stop - start) // unroll
    assert trips * unroll == stop - start

    def step(i, carry):
        for k in range(unroll):
            body(start + i * unroll + k)
        return carry

    if trips == 1:
        step(0, 0)
    else:
        lax.fori_loop(0, trips, step, 0)


def lanes(shape):
    return lax.broadcasted_iota(jnp.int32, shape, len(shape) - 1)


def kernel(
    shift_hbm, src_hbm, mats_hbm, hxy_hbm, lam_hbm, out,
    shift_ref, src, mats, hxy, lam, A, W, f1o, LR1, LR0, H0, F1, F0M, F0H,
    G2, U2, V2, T3, TZ2, B1, V1, U1, T1, tmp, TZM, TZH, BM, BH, VM, VH, TM, TH, RM, RHH, R1, D1, E1,
    csem, ss, rs,
):
    gx, gy, gz = lax.axis_index("gx"), lax.axis_index("gy"), lax.axis_index("gz")
    core = lax.rem(gy, 2)

    def peer(dx, dy, dz):
        return (lax.rem(gx + dx % GX, GX), lax.rem(gy + dy % GY, GY), lax.rem(gz + dz % GZ, GZ))

    partner = (gx, gy + 1 - 2 * core, gz)

    barrier = pltpu.get_barrier_semaphore()
    friends = [(d, 0, 0) for d in range(1, 8)]
    friends += [(0, a, b) for a in (0, 2) for b in range(8) if (a, b) != (0, 0)]
    friends += [(0, 1, 0), (0, 3, 0)]
    friends += [(a, 0, b) for a in (1, 7) for b in (1, 7)]
    for f in friends:
        pl.semaphore_signal(barrier, inc=1, device_id=peer(*f), device_id_type=MESH)

    inputs = [
        pltpu.make_async_copy(src_hbm, src, csem.at[3]),
        pltpu.make_async_copy(shift_hbm, shift_ref, csem.at[4]),
    ]
    loads = [
        pltpu.make_async_copy(mats_hbm, mats, csem.at[0]),
        pltpu.make_async_copy(hxy_hbm, hxy, csem.at[1]),
        pltpu.make_async_copy(lam_hbm, lam, csem.at[2]),
    ]
    for load in inputs + loads:
        load.start()

    used = [0]

    def remote(source, target, device):
        k = used[0]
        used[0] += 1
        return pltpu.make_async_remote_copy(
            src_ref=source, dst_ref=target, send_sem=ss.at[k], recv_sem=rs.at[k],
            device_id=device, device_id_type=MESH,
        )

    def wrap(u):
        for j in range(4):
            u[j, 0] = u[j, 32]
            u[j, 33] = u[j, 1]

    def beside2(u, i, n):
        mid = [u[j, pl.ds(i + 1, n)] for j in range(4)]
        sums = []
        for j in range(4):
            s = u[j, pl.ds(i + 2, n)] + u[j, pl.ds(i, n)]
            s = s + (mid[j + 1] if j < 3 else roll(mid[0], -1, 1))
            s = s + (mid[j - 1] if j > 0 else roll(mid[3], 1, 1))
            s = s + roll(mid[j], -1, 2) + roll(mid[j], 1, 2)
            sums.append(s)
        return mid, sums

    def sweep2(u, v, start, stop):
        def body(t):
            i = 4 * t + start
            mid, sums = beside2(u, i, 4)
            for j in range(4):
                g = G2[j, pl.ds(i + 1, 4)]
                v[j, pl.ds(i + 1, 4)] = mid[j] + c[2] * (g - (d[2] * mid[j] - w[2] * sums[j]))

        loop(0, (stop - start) // 4, body, 4)

    def keep3(values, t):
        for jp in range(2):
            s = values[2 * jp] + values[2 * jp + 1]
            T3[jp, 2 * t] = s[0] + s[1]
            T3[jp, 2 * t + 1] = s[2] + s[3]

    def defect2():
        def body(t):
            i = 4 * t
            mid, sums = beside2(V2, i, 4)
            keep3([G2[j, pl.ds(i + 1, 4)] - (d[2] * mid[j] - w[2] * sums[j]) for j in range(4)], t)

        loop(0, 8, body, 4)

    def defect2_zero():
        def body(t):
            mid, sums = beside2(G2, 4 * t, 4)
            keep3([mid[j] - c[2] * (d[2] * mid[j] - w[2] * sums[j]) for j in range(4)], t)

        loop(0, 8, body, 4)

    def solve3(t, weights, start, stop):
        x = T3[...].reshape(256, 128)
        x = mm3(x, mats[WZ], mats[WZL])
        x = left3(hxy[0], hxy[1], x)
        x = x / (lam[...] + shift)
        x = left3(hxy[2], hxy[3], x)
        x = mm3(x, mats[t], mats[t + 1]).reshape(2, 16, 8, 128)
        result = []
        for j in range(4):
            jp, p = divmod(j, 2)

            def y_at(off):
                s, k = divmod(jp + off, 2)
                return roll(x[k], -s, 1)

            rows = weighted(weights[p], y_at)

            def x_at(off):
                low, high = start // 2 + off, stop // 2 + off
                parts = [rows[max(low, 0) : min(high, 16)]]
                if low < 0:
                    parts.insert(0, rows[low % 16 :])
                if high > 16:
                    parts.append(rows[: high - 16])
                return parts[0] if len(parts) == 1 else jnp.concatenate(parts, axis=0)

            pair = [weighted(weights[q], x_at) for q in range(2)]
            result.append(jnp.stack(pair, axis=1).reshape(stop - start, 8, 128))
        return result

    def correct2(zero):
        e = solve3(WP, LINEAR, 0, 20)
        for j in range(4):
            if zero:
                V2[j, 1:21] = c[2] * G2[j, 1:21] + e[j]
            else:
                V2[j, 1:21] = V2[j, 1:21] + e[j]
        sweep2(V2, U2, 2, 18)

    def cycle2_zero():
        defect2_zero()
        correct2(True)

    def restrict12(source, row):
        for x in range(4):
            s = None
            for a in range(2):
                for b in range(2):
                    part = source[2 * x + a, pl.ds(row + b, 4, stride=2), :]
                    s = part if s is None else s + part
            tmp[4 * x : 4 * x + 4] = s
        z = mm2(tmp[...], mats[RZ2])
        row_of = lax.broadcasted_iota(jnp.int32, (16, 128), 0)
        z = jnp.where(lax.div(lanes((16, 128)), 32) == lax.rem(row_of, 4), z, 0.0)
        z = z + roll(z, -1, 0)
        tmp[...] = z + roll(z, -2, 0)

    def gather_first(k):
        A[k, 8:12] = tmp[pl.ds(0, 4, stride=4), :]
        copies = []
        for dx in (4, 3, 5, 2, 6, 1, 7):
            slot = (2 - dx) % 8
            copies.append(remote(A.at[k, pl.ds(8, 4)], A.at[k, pl.ds(4 * slot, 4)], peer(dx, 0, 0)))
        for copy in copies:
            copy.start()
        return copies

    far = {0: 0, 1: 1, 2: 1, 3: 2, 4: 2, 5: 2, 6: 1, 7: 1}
    order = [(a, b) for a in (0, 2) for b in range(8) if (a, b) != (0, 0)]

    def gather_second(k, first):
        for copy in first:
            copy.wait_recv()
        W[k, 1, SLOT : SLOT + 32] = A[k]
        copies = {}
        for a, b in order:
            copies[a, b] = remote(
                A.at[k], W.at[k, (1 - a) % 4, pl.ds(SLOT * ((1 - b) % 8), 32)], peer(0, a, b)
            )
        for a, b in sorted(order, key=lambda o: -far[o[1]]):
            copies[a, b].start()
        return copies

    def gather_third(k, second):
        relays = []

        def relay(a, b):
            g, s = (1 - a) % 4, pl.ds(SLOT * ((1 - b) % 8), 32)
            to = lax.rem(g + 3 + 2 * core, 4)
            relays.append(remote(W.at[k, g, s], W.at[k, to, s], partner))
            relays[-1].start()

        relay(0, 0)
        for a, b in sorted(order, key=lambda o: far[o[1]]):
            second[a, b].wait_recv()
            relay(a, b)
        for copy in relays:
            copy.wait_recv()
        return relays

    def unpack(k):
        group = lax.div(lanes((8, 128)), 32)

        def body(x):
            rows = [W[k, g, pl.ds(x, 8, stride=SLOT), :] for g in range(4)]
            for far in (1, 2):
                low = lax.rem(lax.div(group, far), 2) == 0
                for g in range(4):
                    if g & far == 0:
                        first, second = rows[g], rows[g + far]
                        rows[g] = jnp.where(low, first, roll(second, 32 * far, 1))
                        rows[g + far] = jnp.where(low, roll(first, -32 * far, 1), second)
            for j in range(4):
                G2[j, x + 1] = rows[j]

        loop(0, 32, body, 16)
        wrap(G2)

    def refine21(table, weights):
        x = U2[:, 3:19].reshape(512, 128)
        TZ2[...] = mm2(x, mats[table]).reshape(4, 16, 8, 128)

        def body(t):
            for p in range(2):
                planes = [weighted(weights[p], lambda off: TZ2[j, t + 2 + off]) for j in range(4)]
                for j in range(4):
                    for q in range(2):

                        def y_at(off):
                            s, k = divmod(j + off, 4)
                            return roll(planes[k], -s, 0)

                        B1[2 * t + p, pl.ds(2 * j + q, 4, stride=8), :] = weighted(weights[q], y_at)[0:4]

        loop(0, 12, body, 3)

    def beside1(get, i):
        mid = get(i)
        s = get(i + 1) + get(i - 1)
        s = s + roll(mid, -1, 0) + roll(mid, 1, 0)
        s = s + roll(mid, -1, 1) + roll(mid, 1, 1)
        return mid, s

    def defect_of(mid, s, f, k):
        return f - (d[k] * mid - w[k] * s)

    def beside0(i):
        lane = lanes((32, 128))
        mid = [VM[i, 0:32], VH[i, 0:32]]
        up = [roll(m, -1, 1) for m in mid]
        down = [roll(m, 1, 1) for m in mid]
        sums = []
        for k, ref in enumerate((VM, VH)):
            s = ref[i + 1, 0:32] + ref[i - 1, 0:32]
            s = s + roll(mid[k], -1, 0) + roll(mid[k], 1, 0)
            s = s + jnp.where(lane == 127, up[1 - k], up[k]) + jnp.where(lane == 0, down[1 - k], down[k])
            sums.append(s)
        return mid, sums

    inputs[0].wait()
    loads[0].wait()
    rows = []
    for x in range(8):
        s = None
        for a in range(2):
            for b in range(2):
                part = src[2 * x + a, pl.ds(b, 8, stride=2), :]
                s = part if s is None else s + part
        rows.append(s)
    f1o[...] = mm2(jnp.concatenate(rows, axis=0), mats[RZ1]).reshape(8, 8, 128)
    restrict12(f1o, 0)
    inputs[1].wait()
    shift = shift_ref[0]
    w = [0.25**k for k in range(4)]
    d = [6.0 * w[k] + shift for k in range(3)]
    c = [jnp.max(DAMPING / jnp.full((8, 128), d[k], jnp.float32)) for k in range(3)]

    pl.semaphore_wait(barrier, len(friends))
    pending = []
    first = gather_first(0)
    pending += first
    side = []
    for dy, k in ((1, 0), (3, 1)):
        side.append(remote(f1o, LR1.at[k], peer(0, dy, 0)))
    for dy, k in ((1, 0), (3, 1)):
        side.append(remote(src, LR0.at[k], peer(0, dy, 0)))
    for copy in side:
        copy.start()
    pending += side

    second = gather_second(0, first)
    pending += second.values()

    side[0].wait_recv()
    side[1].wait_recv()
    lane = lanes((8, 8, 128))
    F1[8:16, 8:16] = jnp.where(
        lane < 8,
        roll(LR1[0], 64, 2),
        jnp.where(lane < 72, f1o[...], jnp.where(lane < 80, roll(LR1[1], 64, 2), 0.0)),
    )
    corner1 = []
    around = [(1, 0), (-1, 0), (0, 1), (0, -1), (1, 1), (1, -1), (-1, 1), (-1, -1)]
    for dx, dz in around:
        corner1.append(
            remote(
                F1.at[pl.ds(8, 8), pl.ds(8, 8)],
                F1.at[pl.ds(8 - 8 * dx, 8), pl.ds(8 - 8 * dz, 8)],
                peer(dx, 0, dz),
            )
        )
    for copy in corner1:
        copy.start()
    pending += corner1

    side[2].wait_recv()
    side[3].wait_recv()

    def halo0(i):
        lane = lanes((16, 128))
        H0[i] = jnp.where(lane < 8, LR0[1, i], jnp.where(lane >= 120, LR0[0, i], 0.0))
        F0M[i + 6, 8:24] = src[i]
        F0H[i + 6, 8:24] = H0[i]

    loop(0, 16, halo0, 2)

    third = gather_third(0, second)
    pending += third

    corner0 = []
    for dx, dz in around:
        n_x, from_x, to_x = {0: (16, 0, 6), 1: (6, 10, 0), -1: (6, 0, 22)}[dx]
        n_y, from_y, to_y = {0: (16, 0, 8), 1: (8, 8, 0), -1: (8, 0, 24)}[dz]
        for source, target in ((src, F0M), (H0, F0H)):
            corner0.append(
                remote(
                    source.at[pl.ds(from_x, n_x), pl.ds(from_y, n_y)],
                    target.at[pl.ds(to_x, n_x), pl.ds(to_y, n_y)],
                    peer(dx, 0, dz),
                )
            )
    for copy in corner0:
        copy.start()
    pending += corner0

    unpack(0)
    loads[1].wait()
    loads[2].wait()

    def sum3(t):
        keep3([G2[j, pl.ds(4 * t + 1, 4)] for j in range(4)], t)

    loop(0, 8, sum3, 2)
    u = solve3(WQ, CUBIC, 0, 32)
    for j in range(4):
        U2[j, 1:33] = u[j]
    wrap(U2)
    sweep2(U2, V2, 0, 32)
    wrap(V2)
    defect2()
    correct2(False)

    refine21(QZ21, CUBIC)
    for copy in corner1:
        copy.wait_recv()

    def pre1(i):
        mid, s = beside1(lambda k: B1[k, 0:24], i)
        V1[i] = mid + c[1] * defect_of(mid, s, F1[i], 1)

    loop(1, 23, pre1, 11)

    def res1(i):
        mid, s = beside1(lambda k: V1[k], i)
        T1[i - 8] = defect_of(mid, s, F1[i], 1)

    loop(8, 16, res1, 8)
    restrict12(T1, 8)
    first = gather_first(1)
    second = gather_second(1, first)
    third = gather_third(1, second)
    pending += first + list(second.values()) + third
    unpack(1)
    cycle2_zero()
    refine21(PZ21, LINEAR)

    def add1(i):
        V1[i] = V1[i] + B1[i, 0:24]

    loop(2, 22, add1, 4)

    def post1(i):
        mid, s = beside1(lambda k: V1[k], i)
        U1[i - 3] = mid + c[1] * defect_of(mid, s, F1[i], 1)

    loop(3, 21, post1, 9)

    u = U1[...].reshape(432, 128)
    TZM[...] = mm2(u, mats[QZ10M]).reshape(18, 24, 128)
    TZH[...] = mm2(u, mats[QZ10H]).reshape(18, 24, 128)

    def cubic0(t):
        for source, target in ((TZM, BM), (TZH, BH)):
            for p in range(2):
                plane = weighted(CUBIC[p], lambda off: source[t + 2 + off])
                at = {off: roll(plane, -(4 + off), 0)[0:16] for off in range(-2, 3)}
                for q in range(2):
                    target[2 * t + p, pl.ds(q, 16, stride=2), :] = weighted(CUBIC[q], at.__getitem__)

    loop(0, 14, cubic0, 2)
    for copy in corner0:
        copy.wait_recv()

    def pre0(i):
        lane = lanes((32, 128))
        refs = (BM, BH)
        mid = [ref[i, 0:32] for ref in refs]
        up = [roll(m, -1, 1) for m in mid]
        down = [roll(m, 1, 1) for m in mid]
        for k, (f, v) in enumerate(((F0M, VM), (F0H, VH))):
            s = refs[k][i + 1, 0:32] + refs[k][i - 1, 0:32]
            s = s + roll(mid[k], -1, 0) + roll(mid[k], 1, 0)
            s = s + jnp.where(lane == 127, up[1 - k], up[k]) + jnp.where(lane == 0, down[1 - k], down[k])
            v[i, 0:32] = mid[k] + c[0] * defect_of(mid[k], s, f[i, 0:32], 0)

    loop(1, 27, pre0, 13)

    def res0(t):
        for a in range(2):
            i = 2 * t + 2 + a
            mid, sums = beside0(i)
            for k, (f, target) in enumerate(((F0M, TM), (F0H, TH))):
                r = defect_of(mid[k], sums[k], f[i, 0:32], 0)
                target[t, 0:32] = r if a == 0 else target[t, 0:32] + r
        for source, target in ((TM, RM), (TH, RHH)):
            target[t, 0:16] = source[t, pl.ds(0, 16, stride=2), :] + source[t, pl.ds(1, 16, stride=2), :]

    loop(0, 12, res0, 6)
    R1[:, 0:16] = (
        mm2(RM[:, 0:16].reshape(192, 128), mats[RZ1]) + mm2(RHH[:, 0:16].reshape(192, 128), mats[RH])
    ).reshape(12, 16, 128)

    def zero1(i):
        D1[i, 0:16] = c[1] * R1[i, 0:16]

    loop(0, 12, zero1, 4)

    def res1b(i):
        mid, s = beside1(lambda k: D1[k, 0:16], i)
        T1[i - 2, 0:16] = defect_of(mid, s, R1[i, 0:16], 1)

    loop(2, 10, res1b, 8)
    restrict12(T1, 4)
    first = gather_first(2)
    second = gather_second(2, first)
    third = gather_third(2, second)
    pending += first + list(second.values()) + third
    unpack(2)
    cycle2_zero()
    refine21(PZ21, LINEAR)

    def add1b(i):
        D1[i, 0:16] = D1[i, 0:16] + B1[i + 6, 4:20]

    loop(0, 12, add1b, 4)
    E1[0, 0:16] = jnp.zeros((16, 128), jnp.float32)
    E1[11, 0:16] = jnp.zeros((16, 128), jnp.float32)

    def post1b(i):
        mid, s = beside1(lambda k: D1[k, 0:16], i)
        E1[i, 0:16] = mid + c[1] * defect_of(mid, s, R1[i, 0:16], 1)

    loop(1, 11, post1b, 10)

    e = E1[:, 0:16].reshape(192, 128)
    TZM[0:12, 0:16] = mm2(e, mats[PZ10M]).reshape(12, 16, 128)
    TZH[0:12, 0:16] = mm2(e, mats[PZ10H]).reshape(12, 16, 128)

    def linear0(t):
        for source, target, v in ((TZM, BM, VM), (TZH, BH, VH)):
            for p in range(2):
                plane = weighted(LINEAR[p], lambda off: source[t + 1 + off, 0:16])
                i = 2 * t + 4 + p
                for q in range(2):
                    target[i, pl.ds(q, 16, stride=2), :] = weighted(LINEAR[q], lambda off: roll(plane, -off, 0))
                v[i, 0:32] = v[i, 0:32] + target[i, 0:32]

    loop(0, 10, linear0, 2)

    def post0(i):
        mid, sums = beside0(i)
        v = mid[0] + c[0] * defect_of(mid[0], sums[0], F0M[i, 0:32], 0)
        out[i - 6] = v[8:24]

    loop(6, 22, post0, 8)
    for copy in pending:
        copy.wait_send()


def solution(mesh):
    mats, hxy, lam = tables()
    f32 = jnp.float32
    vmem = pltpu.VMEM
    scratch = [
        pltpu.SMEM((1,), f32),
        vmem((16, 16, 128), f32),
        vmem((15, 128, 128), jnp.bfloat16),
        vmem((4, 256, 256), jnp.bfloat16),
        vmem((256, 128), f32),
        vmem((3, 32, 128), f32),
        vmem((3, 4, 8 * SLOT, 128), f32),
        vmem((8, 8, 128), f32),
        vmem((2, 8, 8, 128), f32),
        vmem((2, 16, 16, 128), f32),
        vmem((16, 16, 128), f32),
        vmem((24, 24, 128), f32),
        vmem((28, 40, 128), f32),
        vmem((28, 40, 128), f32),
        vmem((4, 34, 8, 128), f32),
        vmem((4, 34, 8, 128), f32),
        vmem((4, 34, 8, 128), f32),
        vmem((2, 16, 8, 128), f32),
        vmem((4, 16, 8, 128), f32),
        vmem((24, 40, 128), f32),
        vmem((24, 24, 128), f32),
        vmem((18, 24, 128), f32),
        vmem((8, 24, 128), f32),
        vmem((16, 128), f32),
        vmem((18, 24, 128), f32),
        vmem((18, 24, 128), f32),
        vmem((28, 40, 128), f32),
        vmem((28, 40, 128), f32),
        vmem((28, 40, 128), f32),
        vmem((28, 40, 128), f32),
        vmem((12, 40, 128), f32),
        vmem((12, 40, 128), f32),
        vmem((12, 24, 128), f32),
        vmem((12, 24, 128), f32),
        vmem((12, 24, 128), f32),
        vmem((12, 24, 128), f32),
        vmem((12, 24, 128), f32),
        pltpu.SemaphoreType.DMA((5,)),
        pltpu.SemaphoreType.DMA((N_SEMS,)),
        pltpu.SemaphoreType.DMA((N_SEMS,)),
    ]

    def step(source, shift):
        return pl.pallas_call(
            kernel,
            out_shape=jax.ShapeDtypeStruct(source.shape, f32),
            in_specs=[
                pl.BlockSpec(memory_space=pl.ANY),
            ]
            * 5,
            out_specs=pl.BlockSpec(memory_space=vmem),
            scratch_shapes=scratch,
            compiler_params=pltpu.CompilerParams(collective_id=0, has_side_effects=True),
            name="fcycle",
        )(shift, source, jnp.asarray(mats), jnp.asarray(hxy), jnp.asarray(lam))

    spec = P("gx", "gz", "gy")
    return jax.shard_map(step, mesh=mesh, in_specs=(spec, P()), out_specs=spec, check_vma=False)
```

```python
import functools
import math

import jax
import jax.numpy as jnp
import ml_dtypes
import numpy as np
from jax import lax
from jax.experimental import pallas as pl
from jax.experimental.pallas import tpu as pltpu
from jax.sharding import PartitionSpec as P

MESH = pl.DeviceIdType.MESH
DAMPING = 6.0 / 7.0
LINEAR = ({-1: 0.25, 0: 0.75}, {0: 0.75, 1: 0.25})
CUBIC = (
    {-2: -5.0 / 128, -1: 35.0 / 128, 0: 105.0 / 128, 1: -7.0 / 128},
    {-1: -7.0 / 128, 0: 105.0 / 128, 1: 35.0 / 128, 2: -5.0 / 128},
)
GX, GY, GZ = 8, 4, 8
N_GATHER = 7 + 2 * 15 + 16
N_SEMS = 3 * N_GATHER + 4 + 24
SLOT = 40


(RZ1, RZ2, RH, QZ21, PZ21, QZ10M, QZ10H, PZ10M, PZ10H, WZ, WZL, WQ, WQL, WP, WPL, PACK, OPEN) = range(17)


def fourier(n):
    j = np.arange(n)
    rows, eig = [np.full(n, math.sqrt(1.0 / n))], [0.0]
    for k in range(1, n // 2):
        for f in (np.cos, np.sin):
            rows.append(math.sqrt(2.0 / n) * f(2 * np.pi * ((k * j) % n) / n))
            eig.append(2 - 2 * np.cos(2 * np.pi * k / n))
    rows.append(math.sqrt(1.0 / n) * np.where(j % 2, -1.0, 1.0))
    eig.append(4.0)
    return np.array(rows), np.array(eig)


def halves(m):
    high = m.astype(ml_dtypes.bfloat16)
    return high, (m - high.astype(np.float64)).astype(ml_dtypes.bfloat16)


def tables():
    m = np.zeros((17, 128, 128))
    for i in range(64):
        for p in range(2):
            m[RZ1, 2 * i + p, 8 + i] = 0.125
    for i in range(32):
        for p in range(2):
            m[RZ2, 8 + 2 * i + p, i::32] = 0.125
    for k in range(4):
        for p in range(2):
            m[RH, 2 * k + p, 72 + k] = 0.125
            m[RH, 120 + 2 * k + p, 4 + k] = 0.125
    for z in range(-8, 72):
        i, p = divmod(z, 2)
        for t, w in ((QZ21, CUBIC[p]), (PZ21, LINEAR[p])):
            for off, weight in w.items():
                m[t, (32 + i + off) % 128, 8 + z] += weight
    for z in range(-8, 136):
        i, p = divmod(z, 2)
        own = 0 <= z < 128
        for t, w in ((QZ10M if own else QZ10H, CUBIC[p]), (PZ10M if own else PZ10H, LINEAR[p])):
            for off, weight in w.items():
                m[t, 8 + i + off, z % 128] += weight
    for y in range(8):
        for t in range(16):
            z = t if t < 8 else 112 + t
            m[PACK, z, 16 * y + t] = m[OPEN, 16 * y + t, z] = 1.0
    hz, ez = fourier(64)
    down = np.zeros((128, 64))
    for z in range(128):
        down[z, z // 2] = 0.125
    m[WZ, :, :64] = down @ hz.T
    for t, weights in ((WQ, CUBIC), (WP, LINEAR)):
        up = np.zeros((64, 128))
        for z in range(128):
            i, p = divmod(z, 2)
            for off, weight in weights[p].items():
                up[(i + off) % 64, z] += weight
        m[t, :64, :] = hz @ up
    mats = m.astype(ml_dtypes.bfloat16)
    for t in (WZ, WQ, WP):
        mats[t], mats[t + 1] = halves(m[t])
    h, e = fourier(16)
    hxy = np.zeros((256, 256))
    for r in range(256):
        jp, x, g = r // 128, (r // 8) % 16, r % 8
        hxy[:, r] = np.kron(h[:, x], h[:, 2 * g + jp])
    both = np.stack([*halves(hxy), *halves(hxy.T)])
    lam = np.ones((256, 128))
    lam[:, :64] = 0.25**3 * ((e[:, None] + e[None, :]).reshape(256, 1) + ez[None, :])
    return mats, both, lam.astype(np.float32)


def dot(a, b):
    return jnp.dot(a, b, preferred_element_type=jnp.float32)


def split(x):
    high = x.astype(jnp.bfloat16)
    return high, (x - high.astype(jnp.float32)).astype(jnp.bfloat16)


def mm2(x, w):
    high, low = split(x)
    return dot(high, w) + dot(low, w)


def mm3(x, w, w_low):
    high, low = split(x)
    return dot(high, w) + dot(low, w) + dot(high, w_low)


def left3(w, w_low, x):
    high, low = split(x)
    return dot(w, high) + dot(w, low) + dot(w_low, high)


def roll(x, shift, axis):
    shift %= x.shape[axis]
    return x if shift == 0 else pltpu.roll(x, shift, axis)


def weighted(weights, at):
    total = None
    for off, weight in weights.items():
        term = weight * at(off)
        total = term if total is None else total + term
    return total


def loop(start, stop, body, unroll=1):
    trips = (stop - start) // unroll
    assert trips * unroll == stop - start

    def step(i, carry):
        for k in range(unroll):
            body(start + i * unroll + k)
        return carry

    if trips == 1:
        step(0, 0)
    else:
        lax.fori_loop(0, trips, step, 0)


def lanes(shape):
    return lax.broadcasted_iota(jnp.int32, shape, len(shape) - 1)


def kernel(
    shift_hbm, src_hbm, mats_hbm, hxy_hbm, lam_hbm, out,
    shift_ref, src, mats, hxy, lam, A, W, f1o, LR1, LR0, PK, HP, F1, F0M, F0H,
    G2, U2, V2, T3, TZ2, B1, V1, U1, T1, tmp, TZM, TZH, BM, BH, VM, VH, TM, TH, RM, RHH, R1, D1, E1,
    csem, ss, rs,
):
    gx, gy, gz = lax.axis_index("gx"), lax.axis_index("gy"), lax.axis_index("gz")
    core = lax.rem(gy, 2)

    def peer(dx, dy, dz):
        return (lax.rem(gx + dx % GX, GX), lax.rem(gy + dy % GY, GY), lax.rem(gz + dz % GZ, GZ))

    partner = (gx, gy + 1 - 2 * core, gz)

    x_hi = lax.rem(gz, 2)
    turn = 1 - 2 * x_hi
    order = [(lo, hi, dy) for lo in range(2) for hi in range(2) for dy in range(4)]

    def steps(o):
        return ((0, 1), (2, 1))[o[1]][o[0]] + min(o[2], 4 - o[2])

    order.sort(key=steps)
    order = order[1:]
    PARTS = ((0, 16, (3, 5, 6)), (16, 16, (0, 1, 2, 4)))

    barrier = pltpu.get_barrier_semaphore()
    friends = [(d, 0, 0) for d in range(1, 8)]
    friends += [(0, a, b) for a in (0, 2) for b in range(8) if (a, b) != (0, 0)]
    friends += [(0, 1, 0), (0, 3, 0)]
    friends += [(a, 0, b) for a in (1, 7) for b in (1, 7)]
    for f in friends:
        pl.semaphore_signal(barrier, inc=1, device_id=peer(*f), device_id_type=MESH)

    inputs = [
        pltpu.make_async_copy(src_hbm, src, csem.at[3]),
        pltpu.make_async_copy(shift_hbm, shift_ref, csem.at[4]),
    ]
    loads = [
        pltpu.make_async_copy(mats_hbm, mats, csem.at[0]),
        pltpu.make_async_copy(hxy_hbm, hxy, csem.at[1]),
        pltpu.make_async_copy(lam_hbm, lam, csem.at[2]),
    ]
    for load in inputs + loads:
        load.start()

    used = [0]

    def remote(source, target, device):
        k = used[0]
        used[0] += 1
        return pltpu.make_async_remote_copy(
            src_ref=source, dst_ref=target, send_sem=ss.at[k], recv_sem=rs.at[k],
            device_id=device, device_id_type=MESH,
        )

    def wrap(u):
        for j in range(4):
            u[j, 0] = u[j, 32]
            u[j, 33] = u[j, 1]

    def beside2(u, i, n):
        mid = [u[j, pl.ds(i + 1, n)] for j in range(4)]
        sums = []
        for j in range(4):
            s = u[j, pl.ds(i + 2, n)] + u[j, pl.ds(i, n)]
            s = s + (mid[j + 1] if j < 3 else roll(mid[0], -1, 1))
            s = s + (mid[j - 1] if j > 0 else roll(mid[3], 1, 1))
            s = s + roll(mid[j], -1, 2) + roll(mid[j], 1, 2)
            sums.append(s)
        return mid, sums

    def sweep2(u, v, start, stop):
        def body(t):
            i = 4 * t + start
            mid, sums = beside2(u, i, 4)
            for j in range(4):
                g = G2[j, pl.ds(i + 1, 4)]
                v[j, pl.ds(i + 1, 4)] = mid[j] + c[2] * (g - (d[2] * mid[j] - w[2] * sums[j]))

        loop(0, (stop - start) // 4, body, 4)

    def keep3(values, t):
        for jp in range(2):
            s = values[2 * jp] + values[2 * jp + 1]
            T3[jp, 2 * t] = s[0] + s[1]
            T3[jp, 2 * t + 1] = s[2] + s[3]

    def defect2():
        def body(t):
            i = 4 * t
            mid, sums = beside2(V2, i, 4)
            keep3([G2[j, pl.ds(i + 1, 4)] - (d[2] * mid[j] - w[2] * sums[j]) for j in range(4)], t)

        loop(0, 8, body, 4)

    def defect2_zero():
        def body(t):
            mid, sums = beside2(G2, 4 * t, 4)
            keep3([mid[j] - c[2] * (d[2] * mid[j] - w[2] * sums[j]) for j in range(4)], t)

        loop(0, 8, body, 4)

    def solve3(t, weights, start, stop):
        x = T3[...].reshape(256, 128)
        x = mm3(x, mats[WZ], mats[WZL])
        x = left3(hxy[0], hxy[1], x)
        x = x / (lam[...] + shift)
        x = left3(hxy[2], hxy[3], x)
        x = mm3(x, mats[t], mats[t + 1]).reshape(2, 16, 8, 128)
        result = []
        for j in range(4):
            jp, p = divmod(j, 2)

            def y_at(off):
                s, k = divmod(jp + off, 2)
                return roll(x[k], -s, 1)

            rows = weighted(weights[p], y_at)

            def x_at(off):
                low, high = start // 2 + off, stop // 2 + off
                parts = [rows[max(low, 0) : min(high, 16)]]
                if low < 0:
                    parts.insert(0, rows[low % 16 :])
                if high > 16:
                    parts.append(rows[: high - 16])
                return parts[0] if len(parts) == 1 else jnp.concatenate(parts, axis=0)

            pair = [weighted(weights[q], x_at) for q in range(2)]
            result.append(jnp.stack(pair, axis=1).reshape(stop - start, 8, 128))
        return result

    def correct2(zero):
        e = solve3(WP, LINEAR, 0, 20)
        for j in range(4):
            if zero:
                V2[j, 1:21] = c[2] * G2[j, 1:21] + e[j]
            else:
                V2[j, 1:21] = V2[j, 1:21] + e[j]
        sweep2(V2, U2, 2, 18)

    def cycle2_zero():
        defect2_zero()
        correct2(True)

    def restrict12(source, row):
        for x in range(4):
            s = None
            for a in range(2):
                for b in range(2):
                    part = source[2 * x + a, pl.ds(row + b, 4, stride=2), :]
                    s = part if s is None else s + part
            tmp[4 * x : 4 * x + 4] = s
        z = mm2(tmp[...], mats[RZ2])
        row_of = lax.broadcasted_iota(jnp.int32, (16, 128), 0)
        z = jnp.where(lax.div(lanes((16, 128)), 32) == lax.rem(row_of, 4), z, 0.0)
        z = z + roll(z, -1, 0)
        tmp[...] = z + roll(z, -2, 0)

    def gather_first(k):
        A[k, 8:12] = tmp[pl.ds(0, 4, stride=4), :]
        copies = []
        for dx in (4, 3, 5, 2, 6, 1, 7):
            slot = (2 - dx) % 8
            copies.append(remote(A.at[k, pl.ds(8, 4)], A.at[k, pl.ds(4 * slot, 4)], peer(dx, 0, 0)))
        for copy in copies:
            copy.start()
        return copies

    def gather_second(k, first):
        copies = {}
        for part, (row, n, needed) in enumerate(PARTS):
            for i in needed:
                first[i].wait_recv()
            W[k, 1, SLOT + row : SLOT + row + n] = A[k, row : row + n]
            for o in reversed(order):
                lo, hi, dy = o
                rows = pl.ds(SLOT * lax.rem(1 - 2 * dy - hi * turn + 2 * GZ, GZ) + row, n)
                device = (gx, lax.rem(gy + 2 * lo, GY), lax.rem(gz + 2 * dy + hi * turn + GZ, GZ))
                copies[o, part] = remote(A.at[k, pl.ds(row, n)], W.at[k, (1 - 2 * lo) % GY, rows], device)
                copies[o, part].start()
        return copies

    def gather_third(k, second):
        relays = []

        def relay(lo, hi, dy):
            g = (1 - 2 * lo) % 4
            s = pl.ds(SLOT * lax.rem(1 - 2 * dy + hi * turn + 2 * GZ, GZ), 32)
            to = lax.rem(g + 3 + 2 * core, 4)
            relays.append(remote(W.at[k, g, s], W.at[k, to, s], partner))
            relays[-1].start()

        relay(0, 0, 0)
        for o in order:
            for part in range(len(PARTS)):
                second[o, part].wait_recv()
            relay(*o)
        for copy in relays:
            copy.wait_recv()
        return relays

    def unpack(k):
        group = lax.div(lanes((8, 128)), 32)

        def body(x):
            rows = [W[k, g, pl.ds(x, 8, stride=SLOT), :] for g in range(4)]
            for far in (1, 2):
                low = lax.rem(lax.div(group, far), 2) == 0
                for g in range(4):
                    if g & far == 0:
                        first, second = rows[g], rows[g + far]
                        rows[g] = jnp.where(low, first, roll(second, 32 * far, 1))
                        rows[g + far] = jnp.where(low, roll(first, -32 * far, 1), second)
            for j in range(4):
                G2[j, x + 1] = rows[j]

        loop(0, 32, body, 16)
        wrap(G2)

    def refine21(table, weights):
        x = U2[:, 3:19].reshape(512, 128)
        TZ2[...] = mm2(x, mats[table]).reshape(4, 16, 8, 128)

        def body(t):
            for p in range(2):
                planes = [weighted(weights[p], lambda off: TZ2[j, t + 2 + off]) for j in range(4)]
                for j in range(4):
                    for q in range(2):

                        def y_at(off):
                            s, k = divmod(j + off, 4)
                            return roll(planes[k], -s, 0)

                        B1[2 * t + p, pl.ds(2 * j + q, 4, stride=8), :] = weighted(weights[q], y_at)[0:4]

        loop(0, 12, body, 3)

    def beside1(get, i):
        mid = get(i)
        s = get(i + 1) + get(i - 1)
        s = s + roll(mid, -1, 0) + roll(mid, 1, 0)
        s = s + roll(mid, -1, 1) + roll(mid, 1, 1)
        return mid, s

    def defect_of(mid, s, f, k):
        return f - (d[k] * mid - w[k] * s)

    def beside0(i):
        lane = lanes((32, 128))
        mid = [VM[i, 0:32], VH[i, 0:32]]
        up = [roll(m, -1, 1) for m in mid]
        down = [roll(m, 1, 1) for m in mid]
        sums = []
        for k, ref in enumerate((VM, VH)):
            s = ref[i + 1, 0:32] + ref[i - 1, 0:32]
            s = s + roll(mid[k], -1, 0) + roll(mid[k], 1, 0)
            s = s + jnp.where(lane == 127, up[1 - k], up[k]) + jnp.where(lane == 0, down[1 - k], down[k])
            sums.append(s)
        return mid, sums

    inputs[0].wait()
    loads[0].wait()
    rows = []
    for x in range(8):
        s = None
        for a in range(2):
            for b in range(2):
                part = src[2 * x + a, pl.ds(b, 8, stride=2), :]
                s = part if s is None else s + part
        rows.append(s)
    f1o[...] = mm2(jnp.concatenate(rows, axis=0), mats[RZ1]).reshape(8, 8, 128)
    restrict12(f1o, 0)
    inputs[1].wait()
    shift = shift_ref[0]
    w = [0.25**k for k in range(4)]
    d = [6.0 * w[k] + shift for k in range(3)]
    c = [jnp.max(DAMPING / jnp.full((8, 128), d[k], jnp.float32)) for k in range(3)]

    ends = mm2(src[...].reshape(256, 128), mats[PACK]).reshape(16, 2, 8, 128)
    spot = lax.div(lanes((16, 8, 128)), 16) == lax.broadcasted_iota(jnp.int32, (16, 8, 128), 1)
    for y in range(2):
        PK[y] = jnp.sum(jnp.where(spot, ends[:, y], 0.0), axis=1)
    pl.semaphore_wait(barrier, len(friends))
    pending = []
    first = gather_first(0)
    pending += first
    side = []
    for dy, k in ((1, 0), (3, 1)):
        side.append(remote(f1o, LR1.at[k], peer(0, dy, 0)))
    for dy, k in ((1, 0), (3, 1)):
        side.append(remote(PK, LR0.at[k], peer(0, dy, 0)))
    for copy in side:
        copy.start()
    pending += side

    second = gather_second(0, first)
    pending += second.values()

    side[0].wait_recv()
    side[1].wait_recv()
    lane = lanes((8, 8, 128))
    F1[8:16, 8:16] = jnp.where(
        lane < 8,
        roll(LR1[0], 64, 2),
        jnp.where(lane < 72, f1o[...], jnp.where(lane < 80, roll(LR1[1], 64, 2), 0.0)),
    )
    corner1 = []
    around = [(1, 0), (-1, 0), (0, 1), (0, -1), (1, 1), (1, -1), (-1, 1), (-1, -1)]
    for dx, dz in around:
        (n_x, from_x, to_x), (n_y, from_y, to_y) = (
            {0: (8, 8, 8), 1: (6, 10, 2), -1: (6, 8, 16)}[step] for step in (dx, dz)
        )
        corner1.append(
            remote(
                F1.at[pl.ds(from_x, n_x), pl.ds(from_y, n_y)],
                F1.at[pl.ds(to_x, n_x), pl.ds(to_y, n_y)],
                peer(dx, 0, dz),
            )
        )
    for copy in corner1:
        copy.start()
    pending += corner1

    side[2].wait_recv()
    side[3].wait_recv()

    after = lax.rem(lanes((2, 16, 128)), 16) < 8
    HP[1:3, 6:22] = jnp.where(after, LR0[1], LR0[0])
    F0M[6:22, 8:24] = src[...]

    third = gather_third(0, second)
    pending += third

    corner0, packed0 = [], []
    for dx, dz in around:
        n_x, from_x, to_x = {0: (16, 0, 6), 1: (5, 11, 1), -1: (5, 0, 22)}[dx]
        n_y, from_y, to_y = {0: (16, 0, 8), 1: (6, 10, 2), -1: (6, 0, 24)}[dz]
        corner0.append(
            remote(
                src.at[pl.ds(from_x, n_x), pl.ds(from_y, n_y)],
                F0M.at[pl.ds(to_x, n_x), pl.ds(to_y, n_y)],
                peer(dx, 0, dz),
            )
        )
        n_g, from_g, to_g = {0: (2, 1, 1), 1: (1, 2, 0), -1: (1, 1, 3)}[dz]
        packed0.append(
            remote(
                HP.at[pl.ds(from_g, n_g), pl.ds(from_x + 6, n_x)],
                HP.at[pl.ds(to_g, n_g), pl.ds(to_x, n_x)],
                peer(dx, 0, dz),
            )
        )
    for copy in packed0 + corner0:
        copy.start()
    pending += packed0 + corner0

    unpack(0)
    loads[1].wait()
    loads[2].wait()

    def sum3(t):
        keep3([G2[j, pl.ds(4 * t + 1, 4)] for j in range(4)], t)

    loop(0, 8, sum3, 2)
    u = solve3(WQ, CUBIC, 0, 32)
    for j in range(4):
        U2[j, 1:33] = u[j]
    wrap(U2)
    sweep2(U2, V2, 0, 32)
    wrap(V2)
    defect2()
    correct2(False)

    refine21(QZ21, CUBIC)
    for copy in corner1:
        copy.wait_recv()

    def pre1(i):
        mid, s = beside1(lambda k: B1[k, 0:24], i)
        V1[i] = mid + c[1] * defect_of(mid, s, F1[i], 1)

    loop(2, 22, pre1, 10)

    def res1(i):
        mid, s = beside1(lambda k: V1[k], i)
        T1[i - 8] = defect_of(mid, s, F1[i], 1)

    loop(8, 16, res1, 8)
    restrict12(T1, 8)
    first = gather_first(1)
    second = gather_second(1, first)
    for copy in packed0:
        copy.wait_recv()

    def open0(i):
        spot = lax.div(lanes((4, 8, 128)), 16) == lax.broadcasted_iota(jnp.int32, (4, 8, 128), 1)
        rows = jnp.where(spot, jnp.broadcast_to(HP[:, i].reshape(4, 1, 128), (4, 8, 128)), 0.0)
        BH[i, 0:32] = rows.reshape(32, 128)

    loop(1, 27, open0, 2)
    F0H[1:27, 0:32] = mm2(BH[1:27, 0:32].reshape(832, 128), mats[OPEN]).reshape(26, 32, 128)
    third = gather_third(1, second)
    pending += first + list(second.values()) + third
    unpack(1)
    cycle2_zero()
    refine21(PZ21, LINEAR)

    def add1(i):
        V1[i] = V1[i] + B1[i, 0:24]

    loop(2, 22, add1, 4)

    def post1(i):
        mid, s = beside1(lambda k: V1[k], i)
        U1[i - 3] = mid + c[1] * defect_of(mid, s, F1[i], 1)

    loop(3, 21, post1, 9)

    u = U1[...].reshape(432, 128)
    TZM[...] = mm2(u, mats[QZ10M]).reshape(18, 24, 128)
    TZH[...] = mm2(u, mats[QZ10H]).reshape(18, 24, 128)

    def cubic0(t):
        for source, target in ((TZM, BM), (TZH, BH)):
            for p in range(2):
                plane = weighted(CUBIC[p], lambda off: source[t + 2 + off])
                at = {off: roll(plane, -(4 + off), 0)[0:16] for off in range(-2, 3)}
                for q in range(2):
                    target[2 * t + p, pl.ds(q, 16, stride=2), :] = weighted(CUBIC[q], at.__getitem__)

    loop(0, 14, cubic0, 2)
    for copy in corner0:
        copy.wait_recv()

    def pre0(i):
        lane = lanes((32, 128))
        refs = (BM, BH)
        mid = [ref[i, 0:32] for ref in refs]
        up = [roll(m, -1, 1) for m in mid]
        down = [roll(m, 1, 1) for m in mid]
        for k, (f, v) in enumerate(((F0M, VM), (F0H, VH))):
            s = refs[k][i + 1, 0:32] + refs[k][i - 1, 0:32]
            s = s + roll(mid[k], -1, 0) + roll(mid[k], 1, 0)
            s = s + jnp.where(lane == 127, up[1 - k], up[k]) + jnp.where(lane == 0, down[1 - k], down[k])
            v[i, 0:32] = mid[k] + c[0] * defect_of(mid[k], s, f[i, 0:32], 0)

    loop(1, 27, pre0, 13)

    def res0(t):
        for a in range(2):
            i = 2 * t + 2 + a
            mid, sums = beside0(i)
            for k, (f, target) in enumerate(((F0M, TM), (F0H, TH))):
                r = defect_of(mid[k], sums[k], f[i, 0:32], 0)
                target[t, 0:32] = r if a == 0 else target[t, 0:32] + r
        for source, target in ((TM, RM), (TH, RHH)):
            target[t, 0:16] = source[t, pl.ds(0, 16, stride=2), :] + source[t, pl.ds(1, 16, stride=2), :]

    loop(0, 12, res0, 6)
    R1[:, 0:16] = (
        mm2(RM[:, 0:16].reshape(192, 128), mats[RZ1]) + mm2(RHH[:, 0:16].reshape(192, 128), mats[RH])
    ).reshape(12, 16, 128)

    def zero1(i):
        D1[i, 0:16] = c[1] * R1[i, 0:16]

    loop(0, 12, zero1, 4)

    def res1b(i):
        mid, s = beside1(lambda k: D1[k, 0:16], i)
        T1[i - 2, 0:16] = defect_of(mid, s, R1[i, 0:16], 1)

    loop(2, 10, res1b, 8)
    restrict12(T1, 4)
    first = gather_first(2)
    second = gather_second(2, first)
    third = gather_third(2, second)
    pending += first + list(second.values()) + third
    unpack(2)
    cycle2_zero()
    refine21(PZ21, LINEAR)

    def add1b(i):
        D1[i, 0:16] = D1[i, 0:16] + B1[i + 6, 4:20]

    loop(0, 12, add1b, 4)
    E1[0, 0:16] = jnp.zeros((16, 128), jnp.float32)
    E1[11, 0:16] = jnp.zeros((16, 128), jnp.float32)

    def post1b(i):
        mid, s = beside1(lambda k: D1[k, 0:16], i)
        E1[i, 0:16] = mid + c[1] * defect_of(mid, s, R1[i, 0:16], 1)

    loop(1, 11, post1b, 10)

    e = E1[:, 0:16].reshape(192, 128)
    TZM[0:12, 0:16] = mm2(e, mats[PZ10M]).reshape(12, 16, 128)
    TZH[0:12, 0:16] = mm2(e, mats[PZ10H]).reshape(12, 16, 128)

    def linear0(t):
        for source, target, v in ((TZM, BM, VM), (TZH, BH, VH)):
            for p in range(2):
                plane = weighted(LINEAR[p], lambda off: source[t + 1 + off, 0:16])
                i = 2 * t + 4 + p
                for q in range(2):
                    target[i, pl.ds(q, 16, stride=2), :] = weighted(LINEAR[q], lambda off: roll(plane, -off, 0))
                v[i, 0:32] = v[i, 0:32] + target[i, 0:32]

    loop(0, 10, linear0, 2)

    def post0(i):
        mid, sums = beside0(i)
        v = mid[0] + c[0] * defect_of(mid[0], sums[0], F0M[i, 0:32], 0)
        out[i - 6] = v[8:24]

    loop(6, 22, post0, 8)
    for copy in pending:
        copy.wait_send()


def solution(mesh):
    mats, hxy, lam = tables()
    f32 = jnp.float32
    vmem = pltpu.VMEM
    scratch = [
        pltpu.SMEM((1,), f32),
        vmem((16, 16, 128), f32),
        vmem((17, 128, 128), jnp.bfloat16),
        vmem((4, 256, 256), jnp.bfloat16),
        vmem((256, 128), f32),
        vmem((3, 32, 128), f32),
        vmem((3, 4, 8 * SLOT, 128), f32),
        vmem((8, 8, 128), f32),
        vmem((2, 8, 8, 128), f32),
        vmem((2, 2, 16, 128), f32),
        vmem((2, 16, 128), f32),
        vmem((4, 28, 128), f32),
        vmem((24, 24, 128), f32),
        vmem((28, 40, 128), f32),
        vmem((28, 40, 128), f32),
        vmem((4, 34, 8, 128), f32),
        vmem((4, 34, 8, 128), f32),
        vmem((4, 34, 8, 128), f32),
        vmem((2, 16, 8, 128), f32),
        vmem((4, 16, 8, 128), f32),
        vmem((24, 40, 128), f32),
        vmem((24, 24, 128), f32),
        vmem((18, 24, 128), f32),
        vmem((8, 24, 128), f32),
        vmem((16, 128), f32),
        vmem((18, 24, 128), f32),
        vmem((18, 24, 128), f32),
        vmem((28, 40, 128), f32),
        vmem((28, 40, 128), f32),
        vmem((28, 40, 128), f32),
        vmem((28, 40, 128), f32),
        vmem((12, 40, 128), f32),
        vmem((12, 40, 128), f32),
        vmem((12, 24, 128), f32),
        vmem((12, 24, 128), f32),
        vmem((12, 24, 128), f32),
        vmem((12, 24, 128), f32),
        vmem((12, 24, 128), f32),
        pltpu.SemaphoreType.DMA((5,)),
        pltpu.SemaphoreType.DMA((N_SEMS,)),
        pltpu.SemaphoreType.DMA((N_SEMS,)),
    ]

    def step(source, shift):
        return pl.pallas_call(
            kernel,
            out_shape=jax.ShapeDtypeStruct(source.shape, f32),
            in_specs=[
                pl.BlockSpec(memory_space=pl.ANY),
            ]
            * 5,
            out_specs=pl.BlockSpec(memory_space=vmem),
            scratch_shapes=scratch,
            compiler_params=pltpu.CompilerParams(collective_id=0, has_side_effects=True),
            name="fcycle",
        )(shift, source, jnp.asarray(mats), jnp.asarray(hxy), jnp.asarray(lam))

    spec = P("gx", "gz", "gy")
    return jax.shard_map(step, mesh=mesh, in_specs=(spec, P()), out_specs=spec, check_vma=False)
```

```python
import functools
import math

import jax
import jax.numpy as jnp
import ml_dtypes
import numpy as np
from jax import lax
from jax.experimental import pallas as pl
from jax.experimental.pallas import tpu as pltpu
from jax.sharding import PartitionSpec as P

MESH = pl.DeviceIdType.MESH
DAMPING = 6.0 / 7.0
LINEAR = ({-1: 0.25, 0: 0.75}, {0: 0.75, 1: 0.25})
CUBIC = (
    {-2: -5.0 / 128, -1: 35.0 / 128, 0: 105.0 / 128, 1: -7.0 / 128},
    {-1: -7.0 / 128, 0: 105.0 / 128, 1: 35.0 / 128, 2: -5.0 / 128},
)
GX, GY, GZ = 8, 4, 8
N_GATHER = 7 + 2 * 15 + 16
N_SEMS = 3 * N_GATHER + 4 + 24
SLOT = 40


(RZ1, RZ2, RH, QZ21, PZ21, QZ10M, QZ10H, PZ10M, PZ10H, WZ, WZL, WQ, WQL, WP, WPL, PACK, OPEN) = range(17)


def fourier(n):
    j = np.arange(n)
    rows, eig = [np.full(n, math.sqrt(1.0 / n))], [0.0]
    for k in range(1, n // 2):
        for f in (np.cos, np.sin):
            rows.append(math.sqrt(2.0 / n) * f(2 * np.pi * ((k * j) % n) / n))
            eig.append(2 - 2 * np.cos(2 * np.pi * k / n))
    rows.append(math.sqrt(1.0 / n) * np.where(j % 2, -1.0, 1.0))
    eig.append(4.0)
    return np.array(rows), np.array(eig)


def halves(m):
    high = m.astype(ml_dtypes.bfloat16)
    return high, (m - high.astype(np.float64)).astype(ml_dtypes.bfloat16)


def tables():
    m = np.zeros((17, 128, 128))
    for i in range(64):
        for p in range(2):
            m[RZ1, 2 * i + p, 8 + i] = 0.125
    for i in range(32):
        for p in range(2):
            m[RZ2, 8 + 2 * i + p, i::32] = 0.125
    for k in range(4):
        for p in range(2):
            m[RH, 2 * k + p, 72 + k] = 0.125
            m[RH, 120 + 2 * k + p, 4 + k] = 0.125
    for z in range(-8, 72):
        i, p = divmod(z, 2)
        for t, w in ((QZ21, CUBIC[p]), (PZ21, LINEAR[p])):
            for off, weight in w.items():
                m[t, (32 + i + off) % 128, 8 + z] += weight
    for z in range(-8, 136):
        i, p = divmod(z, 2)
        own = 0 <= z < 128
        for t, w in ((QZ10M if own else QZ10H, CUBIC[p]), (PZ10M if own else PZ10H, LINEAR[p])):
            for off, weight in w.items():
                m[t, 8 + i + off, z % 128] += weight
    for y in range(8):
        for t in range(16):
            z = t if t < 8 else 112 + t
            m[PACK, z, 16 * y + t] = m[OPEN, 16 * y + t, z] = 1.0
    hz, ez = fourier(64)
    down = np.zeros((128, 64))
    for z in range(128):
        down[z, z // 2] = 0.125
    m[WZ, :, :64] = down @ hz.T
    for t, weights in ((WQ, CUBIC), (WP, LINEAR)):
        up = np.zeros((64, 128))
        for z in range(128):
            i, p = divmod(z, 2)
            for off, weight in weights[p].items():
                up[(i + off) % 64, z] += weight
        m[t, :64, :] = hz @ up
    mats = m.astype(ml_dtypes.bfloat16)
    for t in (WZ, WQ, WP):
        mats[t], mats[t + 1] = halves(m[t])
    h, e = fourier(16)
    hxy = np.zeros((256, 256))
    for r in range(256):
        jp, x, g = r // 128, (r // 8) % 16, r % 8
        hxy[:, r] = np.kron(h[:, x], h[:, 2 * g + jp])
    both = np.stack([*halves(hxy), *halves(hxy.T)])
    lam = np.ones((256, 128))
    lam[:, :64] = 0.25**3 * ((e[:, None] + e[None, :]).reshape(256, 1) + ez[None, :])
    return mats, both, lam.astype(np.float32)


def dot(a, b):
    return jnp.dot(a, b, preferred_element_type=jnp.float32)


def split(x):
    high = x.astype(jnp.bfloat16)
    return high, (x - high.astype(jnp.float32)).astype(jnp.bfloat16)


def mm2(x, w):
    high, low = split(x)
    return dot(high, w) + dot(low, w)


def mm3(x, w, w_low):
    high, low = split(x)
    return dot(high, w) + dot(low, w) + dot(high, w_low)


def left3(w, w_low, x):
    high, low = split(x)
    return dot(w, high) + dot(w, low) + dot(w_low, high)


def roll(x, shift, axis):
    shift %= x.shape[axis]
    return x if shift == 0 else pltpu.roll(x, shift, axis)


def weighted(weights, at):
    total = None
    for off, weight in weights.items():
        term = weight * at(off)
        total = term if total is None else total + term
    return total


def loop(start, stop, body, unroll=1):
    trips = (stop - start) // unroll
    assert trips * unroll == stop - start

    def step(i, carry):
        for k in range(unroll):
            body(start + i * unroll + k)
        return carry

    if trips == 1:
        step(0, 0)
    else:
        lax.fori_loop(0, trips, step, 0)


def lanes(shape):
    return lax.broadcasted_iota(jnp.int32, shape, len(shape) - 1)


def kernel(
    shift_hbm, src_hbm, mats_hbm, hxy_hbm, lam_hbm, out,
    shift_ref, src, mats, hxy, lam, A, W, f1o, LR1, LR0, PK, HP, F1, F0M, F0H,
    G2, U2, V2, T3, TZ2, B1, V1, U1, T1, tmp, TZM, TZH, BM, BH, VM, VH, TM, TH, RM, RHH, R1, D1, E1,
    csem, ss, rs,
):
    gx, gy, gz = lax.axis_index("gx"), lax.axis_index("gy"), lax.axis_index("gz")
    core = lax.rem(gy, 2)

    def peer(dx, dy, dz):
        return (lax.rem(gx + dx % GX, GX), lax.rem(gy + dy % GY, GY), lax.rem(gz + dz % GZ, GZ))

    partner = (gx, gy + 1 - 2 * core, gz)

    x_hi = lax.rem(gz, 2)
    turn = 1 - 2 * x_hi
    order = [(lo, hi, dy) for lo in range(2) for hi in range(2) for dy in range(4)]

    def steps(o):
        return ((0, 1), (2, 1))[o[1]][o[0]] + min(o[2], 4 - o[2])

    order.sort(key=steps)
    order = order[1:]
    PARTS = ((0, 16, (3, 5, 6)), (16, 16, (0, 1, 2, 4)))

    barrier = pltpu.get_barrier_semaphore()
    friends = [(d, 0, 0) for d in range(1, 8)]
    friends += [(0, a, b) for a in (0, 2) for b in range(8) if (a, b) != (0, 0)]
    friends += [(0, 1, 0), (0, 3, 0)]
    friends += [(a, 0, b) for a in (1, 7) for b in (1, 7)]
    for f in friends:
        pl.semaphore_signal(barrier, inc=1, device_id=peer(*f), device_id_type=MESH)

    inputs = [
        pltpu.make_async_copy(src_hbm, src, csem.at[3]),
        pltpu.make_async_copy(shift_hbm, shift_ref, csem.at[4]),
    ]
    loads = [
        pltpu.make_async_copy(mats_hbm, mats, csem.at[0]),
        pltpu.make_async_copy(hxy_hbm, hxy, csem.at[1]),
        pltpu.make_async_copy(lam_hbm, lam, csem.at[2]),
    ]
    for load in inputs + loads:
        load.start()

    used = [0]

    def remote(source, target, device):
        k = used[0]
        used[0] += 1
        return pltpu.make_async_remote_copy(
            src_ref=source, dst_ref=target, send_sem=ss.at[k], recv_sem=rs.at[k],
            device_id=device, device_id_type=MESH,
        )

    def wrap(u):
        for j in range(4):
            u[j, 0] = u[j, 32]
            u[j, 33] = u[j, 1]

    def beside2(u, i, n):
        mid = [u[j, pl.ds(i + 1, n)] for j in range(4)]
        sums = []
        for j in range(4):
            s = u[j, pl.ds(i + 2, n)] + u[j, pl.ds(i, n)]
            s = s + (mid[j + 1] if j < 3 else roll(mid[0], -1, 1))
            s = s + (mid[j - 1] if j > 0 else roll(mid[3], 1, 1))
            s = s + roll(mid[j], -1, 2) + roll(mid[j], 1, 2)
            sums.append(s)
        return mid, sums

    def sweep2(u, v, start, stop):
        def body(t):
            i = 4 * t + start
            mid, sums = beside2(u, i, 4)
            for j in range(4):
                g = G2[j, pl.ds(i + 1, 4)]
                v[j, pl.ds(i + 1, 4)] = mid[j] + c[2] * (g - (d[2] * mid[j] - w[2] * sums[j]))

        loop(0, (stop - start) // 4, body, 4)

    def keep3(values, t):
        for jp in range(2):
            s = values[2 * jp] + values[2 * jp + 1]
            T3[jp, 2 * t] = s[0] + s[1]
            T3[jp, 2 * t + 1] = s[2] + s[3]

    def defect2():
        def body(t):
            i = 4 * t
            mid, sums = beside2(V2, i, 4)
            keep3([G2[j, pl.ds(i + 1, 4)] - (d[2] * mid[j] - w[2] * sums[j]) for j in range(4)], t)

        loop(0, 8, body, 8)

    def defect2_zero():
        def body(t):
            mid, sums = beside2(G2, 4 * t, 4)
            keep3([mid[j] - c[2] * (d[2] * mid[j] - w[2] * sums[j]) for j in range(4)], t)

        loop(0, 8, body, 8)

    def solve3(t, weights, start, stop):
        x = T3[...].reshape(256, 128)
        x = mm3(x, mats[WZ], mats[WZL])
        x = left3(hxy[0], hxy[1], x)
        x = x / (lam[...] + shift)
        x = left3(hxy[2], hxy[3], x)
        x = mm3(x, mats[t], mats[t + 1]).reshape(2, 16, 8, 128)
        result = []
        for j in range(4):
            jp, p = divmod(j, 2)

            def y_at(off):
                s, k = divmod(jp + off, 2)
                return roll(x[k], -s, 1)

            rows = weighted(weights[p], y_at)

            def x_at(off):
                low, high = start // 2 + off, stop // 2 + off
                parts = [rows[max(low, 0) : min(high, 16)]]
                if low < 0:
                    parts.insert(0, rows[low % 16 :])
                if high > 16:
                    parts.append(rows[: high - 16])
                return parts[0] if len(parts) == 1 else jnp.concatenate(parts, axis=0)

            pair = [weighted(weights[q], x_at) for q in range(2)]
            result.append(jnp.stack(pair, axis=1).reshape(stop - start, 8, 128))
        return result

    def correct2(zero):
        e = solve3(WP, LINEAR, 0, 20)
        for j in range(4):
            if zero:
                V2[j, 1:21] = c[2] * G2[j, 1:21] + e[j]
            else:
                V2[j, 1:21] = V2[j, 1:21] + e[j]
        sweep2(V2, U2, 2, 18)

    def cycle2_zero():
        defect2_zero()
        correct2(True)

    def restrict12(source, row):
        for x in range(4):
            s = None
            for a in range(2):
                for b in range(2):
                    part = source[2 * x + a, pl.ds(row + b, 4, stride=2), :]
                    s = part if s is None else s + part
            tmp[4 * x : 4 * x + 4] = s
        z = mm2(tmp[...], mats[RZ2])
        row_of = lax.broadcasted_iota(jnp.int32, (16, 128), 0)
        z = jnp.where(lax.div(lanes((16, 128)), 32) == lax.rem(row_of, 4), z, 0.0)
        z = z + roll(z, -1, 0)
        tmp[...] = z + roll(z, -2, 0)

    def gather_first(k):
        A[k, 8:12] = tmp[pl.ds(0, 4, stride=4), :]
        copies = []
        for dx in (4, 3, 5, 2, 6, 1, 7):
            slot = (2 - dx) % 8
            copies.append(remote(A.at[k, pl.ds(8, 4)], A.at[k, pl.ds(4 * slot, 4)], peer(dx, 0, 0)))
        for copy in copies:
            copy.start()
        return copies

    def gather_second(k, first):
        copies = {}
        for part, (row, n, needed) in enumerate(PARTS):
            for i in needed:
                first[i].wait_recv()
            W[k, 1, SLOT + row : SLOT + row + n] = A[k, row : row + n]
            for o in reversed(order):
                lo, hi, dy = o
                rows = pl.ds(SLOT * lax.rem(1 - 2 * dy - hi * turn + 2 * GZ, GZ) + row, n)
                device = (gx, lax.rem(gy + 2 * lo, GY), lax.rem(gz + 2 * dy + hi * turn + GZ, GZ))
                copies[o, part] = remote(A.at[k, pl.ds(row, n)], W.at[k, (1 - 2 * lo) % GY, rows], device)
                copies[o, part].start()
        return copies

    def gather_third(k, second):
        relays = []

        def relay(lo, hi, dy):
            g = (1 - 2 * lo) % 4
            s = pl.ds(SLOT * lax.rem(1 - 2 * dy + hi * turn + 2 * GZ, GZ), 32)
            to = lax.rem(g + 3 + 2 * core, 4)
            relays.append(remote(W.at[k, g, s], W.at[k, to, s], partner))
            relays[-1].start()

        relay(0, 0, 0)
        for o in order:
            for part in range(len(PARTS)):
                second[o, part].wait_recv()
            relay(*o)
        for copy in relays:
            copy.wait_recv()
        return relays

    def unpack(k):
        group = lax.div(lanes((8, 128)), 32)

        def body(x):
            rows = [W[k, g, pl.ds(x, 8, stride=SLOT), :] for g in range(4)]
            for far in (1, 2):
                low = lax.rem(lax.div(group, far), 2) == 0
                for g in range(4):
                    if g & far == 0:
                        first, second = rows[g], rows[g + far]
                        rows[g] = jnp.where(low, first, roll(second, 32 * far, 1))
                        rows[g + far] = jnp.where(low, roll(first, -32 * far, 1), second)
            for j in range(4):
                G2[j, x + 1] = rows[j]

        loop(0, 32, body, 32)
        wrap(G2)

    def refine21_z(table):
        x = U2[:, 3:19].reshape(512, 128)
        TZ2[...] = mm2(x, mats[table]).reshape(4, 16, 8, 128)

    def refine21(weights, start, stop):
        def body(t):
            for p in range(2):
                planes = [weighted(weights[p], lambda off: TZ2[j, t + 2 + off]) for j in range(4)]
                for j in range(4):
                    for q in range(2):

                        def y_at(off):
                            s, k = divmod(j + off, 4)
                            return roll(planes[k], -s, 0)

                        B1[2 * t + p, pl.ds(2 * j + q, 4, stride=8), :] = weighted(weights[q], y_at)[0:4]

        loop(start, stop, body, min(6, stop - start))

    def beside1(get, i):
        mid = get(i)
        s = get(i + 1) + get(i - 1)
        s = s + roll(mid, -1, 0) + roll(mid, 1, 0)
        s = s + roll(mid, -1, 1) + roll(mid, 1, 1)
        return mid, s

    def defect_of(mid, s, f, k):
        return f - (d[k] * mid - w[k] * s)

    def beside0(i):
        lane = lanes((32, 128))
        mid = [VM[i, 0:32], VH[i, 0:32]]
        up = [roll(m, -1, 1) for m in mid]
        down = [roll(m, 1, 1) for m in mid]
        sums = []
        for k, ref in enumerate((VM, VH)):
            s = ref[i + 1, 0:32] + ref[i - 1, 0:32]
            s = s + roll(mid[k], -1, 0) + roll(mid[k], 1, 0)
            s = s + jnp.where(lane == 127, up[1 - k], up[k]) + jnp.where(lane == 0, down[1 - k], down[k])
            sums.append(s)
        return mid, sums

    inputs[0].wait()
    loads[0].wait()
    rows = []
    for x in range(8):
        s = None
        for a in range(2):
            for b in range(2):
                part = src[2 * x + a, pl.ds(b, 8, stride=2), :]
                s = part if s is None else s + part
        rows.append(s)
    f1o[...] = mm2(jnp.concatenate(rows, axis=0), mats[RZ1]).reshape(8, 8, 128)
    restrict12(f1o, 0)
    inputs[1].wait()
    shift = shift_ref[0]
    w = [0.25**k for k in range(4)]
    d = [6.0 * w[k] + shift for k in range(3)]
    c = [jnp.max(DAMPING / jnp.full((8, 128), d[k], jnp.float32)) for k in range(3)]

    ends = mm2(src[...].reshape(256, 128), mats[PACK]).reshape(16, 2, 8, 128)
    spot = lax.div(lanes((16, 8, 128)), 16) == lax.broadcasted_iota(jnp.int32, (16, 8, 128), 1)
    for y in range(2):
        PK[y] = jnp.sum(jnp.where(spot, ends[:, y], 0.0), axis=1)
    pl.semaphore_wait(barrier, len(friends))
    pending = []
    first = gather_first(0)
    pending += first
    side = []
    for dy, k in ((1, 0), (3, 1)):
        side.append(remote(f1o, LR1.at[k], peer(0, dy, 0)))
    for dy, k in ((1, 0), (3, 1)):
        side.append(remote(PK, LR0.at[k], peer(0, dy, 0)))
    for copy in side:
        copy.start()
    pending += side

    second = gather_second(0, first)
    pending += second.values()

    side[0].wait_recv()
    side[1].wait_recv()
    lane = lanes((8, 8, 128))
    F1[8:16, 8:16] = jnp.where(
        lane < 8,
        roll(LR1[0], 64, 2),
        jnp.where(lane < 72, f1o[...], jnp.where(lane < 80, roll(LR1[1], 64, 2), 0.0)),
    )
    corner1 = []
    around = [(1, 0), (-1, 0), (0, 1), (0, -1), (1, 1), (1, -1), (-1, 1), (-1, -1)]
    for dx, dz in around:
        (n_x, from_x, to_x), (n_y, from_y, to_y) = (
            {0: (8, 8, 8), 1: (6, 10, 2), -1: (6, 8, 16)}[step] for step in (dx, dz)
        )
        corner1.append(
            remote(
                F1.at[pl.ds(from_x, n_x), pl.ds(from_y, n_y)],
                F1.at[pl.ds(to_x, n_x), pl.ds(to_y, n_y)],
                peer(dx, 0, dz),
            )
        )
    for copy in corner1:
        copy.start()
    pending += corner1

    side[2].wait_recv()
    side[3].wait_recv()

    after = lax.rem(lanes((2, 16, 128)), 16) < 8
    HP[1:3, 6:22] = jnp.where(after, LR0[1], LR0[0])
    F0M[6:22, 8:24] = src[...]

    third = gather_third(0, second)
    pending += third

    corner0, packed0 = [], []
    for dx, dz in around:
        n_x, from_x, to_x = {0: (16, 0, 6), 1: (5, 11, 1), -1: (5, 0, 22)}[dx]
        n_y, from_y, to_y = {0: (16, 0, 8), 1: (6, 10, 2), -1: (6, 0, 24)}[dz]
        corner0.append(
            remote(
                src.at[pl.ds(from_x, n_x), pl.ds(from_y, n_y)],
                F0M.at[pl.ds(to_x, n_x), pl.ds(to_y, n_y)],
                peer(dx, 0, dz),
            )
        )
        n_g, from_g, to_g = {0: (2, 1, 1), 1: (1, 2, 0), -1: (1, 1, 3)}[dz]
        packed0.append(
            remote(
                HP.at[pl.ds(from_g, n_g), pl.ds(from_x + 6, n_x)],
                HP.at[pl.ds(to_g, n_g), pl.ds(to_x, n_x)],
                peer(dx, 0, dz),
            )
        )
    for copy in packed0 + corner0:
        copy.start()
    pending += packed0 + corner0

    unpack(0)
    loads[1].wait()
    loads[2].wait()

    def sum3(t):
        keep3([G2[j, pl.ds(4 * t + 1, 4)] for j in range(4)], t)

    loop(0, 8, sum3, 2)
    u = solve3(WQ, CUBIC, 0, 32)
    for j in range(4):
        U2[j, 1:33] = u[j]
    wrap(U2)
    sweep2(U2, V2, 0, 32)
    wrap(V2)
    defect2()
    correct2(False)

    refine21_z(QZ21)
    refine21(CUBIC, 3, 9)
    for copy in corner1:
        copy.wait_recv()

    def pre1(i):
        mid, s = beside1(lambda k: B1[k, 0:24], i)
        V1[i] = mid + c[1] * defect_of(mid, s, F1[i], 1)

    loop(7, 17, pre1, 10)

    def res1(i):
        mid, s = beside1(lambda k: V1[k], i)
        T1[i - 8] = defect_of(mid, s, F1[i], 1)

    loop(8, 16, res1, 8)
    restrict12(T1, 8)
    first = gather_first(1)
    second = gather_second(1, first)
    refine21(CUBIC, 0, 3)
    refine21(CUBIC, 9, 12)
    loop(2, 7, pre1, 5)
    loop(17, 22, pre1, 5)
    for copy in packed0:
        copy.wait_recv()

    def open0(i):
        spot = lax.div(lanes((4, 8, 128)), 16) == lax.broadcasted_iota(jnp.int32, (4, 8, 128), 1)
        rows = jnp.where(spot, jnp.broadcast_to(HP[:, i].reshape(4, 1, 128), (4, 8, 128)), 0.0)
        BH[i, 0:32] = rows.reshape(32, 128)

    loop(1, 27, open0, 2)
    F0H[1:27, 0:32] = mm2(BH[1:27, 0:32].reshape(832, 128), mats[OPEN]).reshape(26, 32, 128)
    third = gather_third(1, second)
    pending += first + list(second.values()) + third
    unpack(1)
    cycle2_zero()
    refine21_z(PZ21)
    refine21(LINEAR, 0, 12)

    def add1(i):
        V1[i] = V1[i] + B1[i, 0:24]

    loop(2, 22, add1, 4)

    def post1(i):
        mid, s = beside1(lambda k: V1[k], i)
        U1[i - 3] = mid + c[1] * defect_of(mid, s, F1[i], 1)

    loop(3, 21, post1, 9)

    u = U1[...].reshape(432, 128)
    TZM[...] = mm2(u, mats[QZ10M]).reshape(18, 24, 128)
    TZH[...] = mm2(u, mats[QZ10H]).reshape(18, 24, 128)

    def cubic0(t):
        for source, target in ((TZM, BM), (TZH, BH)):
            for p in range(2):
                plane = weighted(CUBIC[p], lambda off: source[t + 2 + off])
                at = {off: roll(plane, -(4 + off), 0)[0:16] for off in range(-2, 3)}
                for q in range(2):
                    target[2 * t + p, pl.ds(q, 16, stride=2), :] = weighted(CUBIC[q], at.__getitem__)

    loop(1, 13, cubic0, 6)
    for copy in corner0:
        copy.wait_recv()

    def pre0(i):
        lane = lanes((32, 128))
        refs = (BM, BH)
        mid = [ref[i, 0:32] for ref in refs]
        up = [roll(m, -1, 1) for m in mid]
        down = [roll(m, 1, 1) for m in mid]
        for k, (f, v) in enumerate(((F0M, VM), (F0H, VH))):
            s = refs[k][i + 1, 0:32] + refs[k][i - 1, 0:32]
            s = s + roll(mid[k], -1, 0) + roll(mid[k], 1, 0)
            s = s + jnp.where(lane == 127, up[1 - k], up[k]) + jnp.where(lane == 0, down[1 - k], down[k])
            v[i, 0:32] = mid[k] + c[0] * defect_of(mid[k], s, f[i, 0:32], 0)

    loop(3, 25, pre0, 22)

    def res0(t):
        for a in range(2):
            i = 2 * t + 2 + a
            mid, sums = beside0(i)
            for k, (f, target) in enumerate(((F0M, TM), (F0H, TH))):
                r = defect_of(mid[k], sums[k], f[i, 0:32], 0)
                target[t, 0:32] = r if a == 0 else target[t, 0:32] + r
        for source, target in ((TM, RM), (TH, RHH)):
            target[t, 0:16] = source[t, pl.ds(0, 16, stride=2), :] + source[t, pl.ds(1, 16, stride=2), :]

    loop(1, 11, res0, 10)
    R1[1:11, 0:16] = (
        mm2(RM[1:11, 0:16].reshape(160, 128), mats[RZ1]) + mm2(RHH[1:11, 0:16].reshape(160, 128), mats[RH])
    ).reshape(10, 16, 128)

    def zero1(i):
        D1[i, 0:16] = c[1] * R1[i, 0:16]

    loop(1, 11, zero1, 5)

    def res1b(i):
        mid, s = beside1(lambda k: D1[k, 0:16], i)
        T1[i - 2, 0:16] = defect_of(mid, s, R1[i, 0:16], 1)

    loop(2, 10, res1b, 8)
    restrict12(T1, 4)
    first = gather_first(2)
    second = gather_second(2, first)
    for t in (0, 13):
        cubic0(t)
    for i in (1, 2, 25, 26):
        pre0(i)
    for t in (0, 11):
        res0(t)
        R1[t, 0:16] = mm2(RM[t, 0:16], mats[RZ1]) + mm2(RHH[t, 0:16], mats[RH])
        zero1(t)
    third = gather_third(2, second)
    pending += first + list(second.values()) + third
    unpack(2)
    cycle2_zero()
    refine21_z(PZ21)
    refine21(LINEAR, 3, 9)

    def add1b(i):
        D1[i, 0:16] = D1[i, 0:16] + B1[i + 6, 4:20]

    loop(0, 12, add1b, 4)
    E1[0, 0:16] = jnp.zeros((16, 128), jnp.float32)
    E1[11, 0:16] = jnp.zeros((16, 128), jnp.float32)

    def post1b(i):
        mid, s = beside1(lambda k: D1[k, 0:16], i)
        E1[i, 0:16] = mid + c[1] * defect_of(mid, s, R1[i, 0:16], 1)

    loop(1, 11, post1b, 10)

    e = E1[:, 0:16].reshape(192, 128)
    TZM[0:12, 0:16] = mm2(e, mats[PZ10M]).reshape(12, 16, 128)
    TZH[0:12, 0:16] = mm2(e, mats[PZ10H]).reshape(12, 16, 128)

    def linear0(t):
        for source, target, v in ((TZM, BM, VM), (TZH, BH, VH)):
            for p in range(2):
                plane = weighted(LINEAR[p], lambda off: source[t + 1 + off, 0:16])
                i = 2 * t + 4 + p
                for q in range(2):
                    target[i, pl.ds(q, 16, stride=2), :] = weighted(LINEAR[q], lambda off: roll(plane, -off, 0))
                v[i, 0:32] = v[i, 0:32] + target[i, 0:32]

    loop(0, 10, linear0, 5)

    def post0(i):
        mid, sums = beside0(i)
        v = mid[0] + c[0] * defect_of(mid[0], sums[0], F0M[i, 0:32], 0)
        out[i - 6] = v[8:24]

    loop(6, 22, post0, 16)
    for copy in pending:
        copy.wait_send()


def solution(mesh):
    mats, hxy, lam = tables()
    f32 = jnp.float32
    vmem = pltpu.VMEM
    scratch = [
        pltpu.SMEM((1,), f32),
        vmem((16, 16, 128), f32),
        vmem((17, 128, 128), jnp.bfloat16),
        vmem((4, 256, 256), jnp.bfloat16),
        vmem((256, 128), f32),
        vmem((3, 32, 128), f32),
        vmem((3, 4, 8 * SLOT, 128), f32),
        vmem((8, 8, 128), f32),
        vmem((2, 8, 8, 128), f32),
        vmem((2, 2, 16, 128), f32),
        vmem((2, 16, 128), f32),
        vmem((4, 28, 128), f32),
        vmem((24, 24, 128), f32),
        vmem((28, 40, 128), f32),
        vmem((28, 40, 128), f32),
        vmem((4, 34, 8, 128), f32),
        vmem((4, 34, 8, 128), f32),
        vmem((4, 34, 8, 128), f32),
        vmem((2, 16, 8, 128), f32),
        vmem((4, 16, 8, 128), f32),
        vmem((24, 40, 128), f32),
        vmem((24, 24, 128), f32),
        vmem((18, 24, 128), f32),
        vmem((8, 24, 128), f32),
        vmem((16, 128), f32),
        vmem((18, 24, 128), f32),
        vmem((18, 24, 128), f32),
        vmem((28, 40, 128), f32),
        vmem((28, 40, 128), f32),
        vmem((28, 40, 128), f32),
        vmem((28, 40, 128), f32),
        vmem((12, 40, 128), f32),
        vmem((12, 40, 128), f32),
        vmem((12, 24, 128), f32),
        vmem((12, 24, 128), f32),
        vmem((12, 24, 128), f32),
        vmem((12, 24, 128), f32),
        vmem((12, 24, 128), f32),
        pltpu.SemaphoreType.DMA((5,)),
        pltpu.SemaphoreType.DMA((N_SEMS,)),
        pltpu.SemaphoreType.DMA((N_SEMS,)),
    ]

    def step(source, shift):
        return pl.pallas_call(
            kernel,
            out_shape=jax.ShapeDtypeStruct(source.shape, f32),
            in_specs=[
                pl.BlockSpec(memory_space=pl.ANY),
            ]
            * 5,
            out_specs=pl.BlockSpec(memory_space=vmem),
            scratch_shapes=scratch,
            compiler_params=pltpu.CompilerParams(collective_id=0, has_side_effects=True),
            name="fcycle",
        )(shift, source, jnp.asarray(mats), jnp.asarray(hxy), jnp.asarray(lam))

    spec = P("gx", "gz", "gy")
    return jax.shard_map(step, mesh=mesh, in_specs=(spec, P()), out_specs=spec, check_vma=False)
```

```python
import functools
import math

import jax
import jax.numpy as jnp
import ml_dtypes
import numpy as np
from jax import lax
from jax.experimental import pallas as pl
from jax.experimental.pallas import tpu as pltpu
from jax.sharding import PartitionSpec as P

MESH = pl.DeviceIdType.MESH
DAMPING = 6.0 / 7.0
LINEAR = ({-1: 0.25, 0: 0.75}, {0: 0.75, 1: 0.25})
CUBIC = (
    {-2: -5.0 / 128, -1: 35.0 / 128, 0: 105.0 / 128, 1: -7.0 / 128},
    {-1: -7.0 / 128, 0: 105.0 / 128, 1: 35.0 / 128, 2: -5.0 / 128},
)
GX, GY, GZ = 8, 4, 8
N_GATHER = 7 + 2 * 15 + 16
N_SEMS = 3 * N_GATHER + 4 + 24
SLOT = 40


(RZ1, RZ2, RH, QZ21, PZ21, QZ10M, QZ10H, PZ10M, PZ10H, WZ, WZL, WQ, WQL, WP, WPL, PACK, OPEN) = range(17)


def fourier(n):
    j = np.arange(n)
    rows, eig = [np.full(n, math.sqrt(1.0 / n))], [0.0]
    for k in range(1, n // 2):
        for f in (np.cos, np.sin):
            rows.append(math.sqrt(2.0 / n) * f(2 * np.pi * ((k * j) % n) / n))
            eig.append(2 - 2 * np.cos(2 * np.pi * k / n))
    rows.append(math.sqrt(1.0 / n) * np.where(j % 2, -1.0, 1.0))
    eig.append(4.0)
    return np.array(rows), np.array(eig)


def halves(m):
    high = m.astype(ml_dtypes.bfloat16)
    return high, (m - high.astype(np.float64)).astype(ml_dtypes.bfloat16)


def tables():
    m = np.zeros((17, 128, 128))
    for i in range(64):
        for p in range(2):
            m[RZ1, 2 * i + p, 8 + i] = 0.125
    for i in range(32):
        for p in range(2):
            m[RZ2, 8 + 2 * i + p, i::32] = 0.125
    for k in range(4):
        for p in range(2):
            m[RH, 2 * k + p, 72 + k] = 0.125
            m[RH, 120 + 2 * k + p, 4 + k] = 0.125
    for z in range(-8, 72):
        i, p = divmod(z, 2)
        for t, w in ((QZ21, CUBIC[p]), (PZ21, LINEAR[p])):
            for off, weight in w.items():
                m[t, (32 + i + off) % 128, 8 + z] += weight
    for z in range(-8, 136):
        i, p = divmod(z, 2)
        own = 0 <= z < 128
        for t, w in ((QZ10M if own else QZ10H, CUBIC[p]), (PZ10M if own else PZ10H, LINEAR[p])):
            for off, weight in w.items():
                m[t, 8 + i + off, z % 128] += weight
    for y in range(8):
        for t in range(16):
            z = t if t < 8 else 112 + t
            m[PACK, z, 16 * y + t] = m[OPEN, 16 * y + t, z] = 1.0
    hz, ez = fourier(64)
    down = np.zeros((128, 64))
    for z in range(128):
        down[z, z // 2] = 0.125
    m[WZ, :, :64] = down @ hz.T
    for t, weights in ((WQ, CUBIC), (WP, LINEAR)):
        up = np.zeros((64, 128))
        for z in range(128):
            i, p = divmod(z, 2)
            for off, weight in weights[p].items():
                up[(i + off) % 64, z] += weight
        m[t, :64, :] = hz @ up
    mats = m.astype(ml_dtypes.bfloat16)
    for t in (WZ, WQ, WP):
        mats[t], mats[t + 1] = halves(m[t])
    h, e = fourier(16)
    hxy = np.zeros((256, 256))
    for r in range(256):
        jp, x, g = r // 128, (r // 8) % 16, r % 8
        hxy[:, r] = np.kron(h[:, x], h[:, 2 * g + jp])
    both = np.stack([*halves(hxy), *halves(hxy.T)])
    lam = np.ones((256, 128))
    lam[:, :64] = 0.25**3 * ((e[:, None] + e[None, :]).reshape(256, 1) + ez[None, :])
    return mats, both, lam.astype(np.float32)


def dot(a, b):
    return jnp.dot(a, b, preferred_element_type=jnp.float32)


def split(x):
    high = x.astype(jnp.bfloat16)
    return high, (x - high.astype(jnp.float32)).astype(jnp.bfloat16)


def mm2(x, w):
    high, low = split(x)
    return dot(high, w) + dot(low, w)


def mm3(x, w, w_low):
    high, low = split(x)
    return dot(high, w) + dot(low, w) + dot(high, w_low)


def left3(w, w_low, x):
    high, low = split(x)
    return dot(w, high) + dot(w, low) + dot(w_low, high)


def roll(x, shift, axis):
    shift %= x.shape[axis]
    return x if shift == 0 else pltpu.roll(x, shift, axis)


def weighted(weights, at):
    total = None
    for off, weight in weights.items():
        term = weight * at(off)
        total = term if total is None else total + term
    return total


def loop(start, stop, body, unroll=1):
    trips = (stop - start) // unroll
    assert trips * unroll == stop - start

    def step(i, carry):
        for k in range(unroll):
            body(start + i * unroll + k)
        return carry

    if trips == 1:
        step(0, 0)
    else:
        lax.fori_loop(0, trips, step, 0)


def lanes(shape):
    return lax.broadcasted_iota(jnp.int32, shape, len(shape) - 1)


def kernel(
    shift_hbm, src_hbm, mats_hbm, hxy_hbm, lam_hbm, out,
    shift_ref, src, mats, hxy, lam, A, W, f1o, LR1, LR0, PK, HP, F1, F0M, F0H,
    G2, U2, V2, T3, TZ2, B1, V1, U1, T1, tmp, TZM, TZH, BM, BH, VM, VH, TM, TH, RM, RHH, R1, D1, E1,
    csem, ss, rs,
):
    gx, gy, gz = lax.axis_index("gx"), lax.axis_index("gy"), lax.axis_index("gz")
    core = lax.rem(gy, 2)

    def peer(dx, dy, dz):
        return (lax.rem(gx + dx % GX, GX), lax.rem(gy + dy % GY, GY), lax.rem(gz + dz % GZ, GZ))

    partner = (gx, gy + 1 - 2 * core, gz)

    x_hi = lax.rem(gz, 2)
    turn = 1 - 2 * x_hi
    order = [(lo, hi, dy) for lo in range(2) for hi in range(2) for dy in range(4)]

    def steps(o):
        return ((0, 1), (2, 1))[o[1]][o[0]] + min(o[2], 4 - o[2])

    order.sort(key=steps)
    order = order[1:]
    PARTS = ((0, 16, (3, 5, 6)), (16, 16, (0, 1, 2, 4)))

    barrier = pltpu.get_barrier_semaphore()
    friends = [(d, 0, 0) for d in range(1, 8)]
    friends += [(0, a, b) for a in (0, 2) for b in range(8) if (a, b) != (0, 0)]
    friends += [(0, 1, 0), (0, 3, 0)]
    friends += [(a, 0, b) for a in (1, 7) for b in (1, 7)]
    for f in friends:
        pl.semaphore_signal(barrier, inc=1, device_id=peer(*f), device_id_type=MESH)

    inputs = [
        pltpu.make_async_copy(src_hbm, src, csem.at[3]),
        pltpu.make_async_copy(shift_hbm, shift_ref, csem.at[4]),
    ]
    loads = [
        pltpu.make_async_copy(mats_hbm, mats, csem.at[0]),
        pltpu.make_async_copy(hxy_hbm, hxy, csem.at[1]),
        pltpu.make_async_copy(lam_hbm, lam, csem.at[2]),
    ]
    for load in inputs + loads:
        load.start()

    used = [0]

    def remote(source, target, device):
        k = used[0]
        used[0] += 1
        return pltpu.make_async_remote_copy(
            src_ref=source, dst_ref=target, send_sem=ss.at[k], recv_sem=rs.at[k],
            device_id=device, device_id_type=MESH,
        )

    def wrap(u):
        for j in range(4):
            u[j, 0] = u[j, 32]
            u[j, 33] = u[j, 1]

    def beside2(u, i, n):
        mid = [u[j, pl.ds(i + 1, n)] for j in range(4)]
        sums = []
        for j in range(4):
            s = u[j, pl.ds(i + 2, n)] + u[j, pl.ds(i, n)]
            s = s + (mid[j + 1] if j < 3 else roll(mid[0], -1, 1))
            s = s + (mid[j - 1] if j > 0 else roll(mid[3], 1, 1))
            s = s + roll(mid[j], -1, 2) + roll(mid[j], 1, 2)
            sums.append(s)
        return mid, sums

    def sweep2(u, v, start, stop):
        def body(t):
            i = 4 * t + start
            mid, sums = beside2(u, i, 4)
            for j in range(4):
                g = G2[j, pl.ds(i + 1, 4)]
                v[j, pl.ds(i + 1, 4)] = mid[j] + c[2] * (g - (d[2] * mid[j] - w[2] * sums[j]))

        loop(0, (stop - start) // 4, body, 4)

    def keep3(values, t):
        for jp in range(2):
            s = values[2 * jp] + values[2 * jp + 1]
            T3[jp, 2 * t] = s[0] + s[1]
            T3[jp, 2 * t + 1] = s[2] + s[3]

    def defect2():
        def body(t):
            i = 4 * t
            mid, sums = beside2(V2, i, 4)
            keep3([G2[j, pl.ds(i + 1, 4)] - (d[2] * mid[j] - w[2] * sums[j]) for j in range(4)], t)

        loop(0, 8, body, 8)

    def defect2_zero():
        def body(t):
            mid, sums = beside2(G2, 4 * t, 4)
            keep3([mid[j] - c[2] * (d[2] * mid[j] - w[2] * sums[j]) for j in range(4)], t)

        loop(0, 8, body, 8)

    def solve3(t, weights, start, stop):
        x = T3[...].reshape(256, 128)
        x = mm3(x, mats[WZ], mats[WZL])
        x = left3(hxy[0], hxy[1], x)
        x = x / (lam[...] + shift)
        x = left3(hxy[2], hxy[3], x)
        x = mm3(x, mats[t], mats[t + 1]).reshape(2, 16, 8, 128)
        result = []
        for j in range(4):
            jp, p = divmod(j, 2)

            def y_at(off):
                s, k = divmod(jp + off, 2)
                return roll(x[k], -s, 1)

            rows = weighted(weights[p], y_at)

            def x_at(off):
                low, high = start // 2 + off, stop // 2 + off
                parts = [rows[max(low, 0) : min(high, 16)]]
                if low < 0:
                    parts.insert(0, rows[low % 16 :])
                if high > 16:
                    parts.append(rows[: high - 16])
                return parts[0] if len(parts) == 1 else jnp.concatenate(parts, axis=0)

            pair = [weighted(weights[q], x_at) for q in range(2)]
            result.append(jnp.stack(pair, axis=1).reshape(stop - start, 8, 128))
        return result

    def correct2(zero):
        e = solve3(WP, LINEAR, 0, 20)
        for j in range(4):
            if zero:
                V2[j, 1:21] = c[2] * G2[j, 1:21] + e[j]
            else:
                V2[j, 1:21] = V2[j, 1:21] + e[j]
        sweep2(V2, U2, 2, 18)

    def cycle2_zero():
        defect2_zero()
        correct2(True)

    def restrict12(source, row):
        for x in range(4):
            s = None
            for a in range(2):
                for b in range(2):
                    part = source[2 * x + a, pl.ds(row + b, 4, stride=2), :]
                    s = part if s is None else s + part
            tmp[4 * x : 4 * x + 4] = s
        z = mm2(tmp[0:16], mats[RZ2])
        row_of = lax.broadcasted_iota(jnp.int32, (16, 128), 0)
        z = jnp.where(lax.div(lanes((16, 128)), 32) == lax.rem(row_of, 4), z, 0.0)
        z = z + roll(z, -1, 0)
        tmp[0:16] = z + roll(z, -2, 0)

    def gather_first(k):
        A[k, 8:12] = tmp[pl.ds(0, 4, stride=4), :]
        copies = []
        for dx in (4, 3, 5, 2, 6, 1, 7):
            slot = (2 - dx) % 8
            copies.append(remote(A.at[k, pl.ds(8, 4)], A.at[k, pl.ds(4 * slot, 4)], peer(dx, 0, 0)))
        for copy in copies:
            copy.start()
        return copies

    def gather_second(k, first):
        copies = {}
        for part, (row, n, needed) in enumerate(PARTS):
            for i in needed:
                first[i].wait_recv()
            W[k, 1, SLOT + row : SLOT + row + n] = A[k, row : row + n]
            for o in reversed(order):
                lo, hi, dy = o
                rows = pl.ds(SLOT * lax.rem(1 - 2 * dy - hi * turn + 2 * GZ, GZ) + row, n)
                device = (gx, lax.rem(gy + 2 * lo, GY), lax.rem(gz + 2 * dy + hi * turn + GZ, GZ))
                copies[o, part] = remote(A.at[k, pl.ds(row, n)], W.at[k, (1 - 2 * lo) % GY, rows], device)
                copies[o, part].start()
        return copies

    def gather_third(k, second):
        relays = []

        def relay(lo, hi, dy):
            g = (1 - 2 * lo) % 4
            s = pl.ds(SLOT * lax.rem(1 - 2 * dy + hi * turn + 2 * GZ, GZ), 32)
            to = lax.rem(g + 3 + 2 * core, 4)
            relays.append(remote(W.at[k, g, s], W.at[k, to, s], partner))
            relays[-1].start()

        relay(0, 0, 0)
        for o in order:
            for part in range(len(PARTS)):
                second[o, part].wait_recv()
            relay(*o)
        for copy in relays:
            copy.wait_recv()
        return relays

    def unpack(k):
        group = lax.div(lanes((8, 128)), 32)

        def body(x):
            rows = [W[k, g, pl.ds(x, 8, stride=SLOT), :] for g in range(4)]
            for far in (1, 2):
                low = lax.rem(lax.div(group, far), 2) == 0
                for g in range(4):
                    if g & far == 0:
                        first, second = rows[g], rows[g + far]
                        rows[g] = jnp.where(low, first, roll(second, 32 * far, 1))
                        rows[g + far] = jnp.where(low, roll(first, -32 * far, 1), second)
            for j in range(4):
                G2[j, x + 1] = rows[j]

        loop(0, 32, body, 32)
        wrap(G2)

    def refine21_z(table):
        x = U2[:, 3:19].reshape(512, 128)
        TZ2[...] = mm2(x, mats[table]).reshape(4, 16, 8, 128)

    def refine21(weights, start, stop):
        def body(t):
            for p in range(2):
                planes = [weighted(weights[p], lambda off: TZ2[j, t + 2 + off]) for j in range(4)]
                for j in range(4):
                    for q in range(2):

                        def y_at(off):
                            s, k = divmod(j + off, 4)
                            return roll(planes[k], -s, 0)

                        B1[2 * t + p, pl.ds(2 * j + q, 4, stride=8), :] = weighted(weights[q], y_at)[0:4]

        loop(start, stop, body, min(6, stop - start))

    def beside1(get, i):
        mid = get(i)
        s = get(i + 1) + get(i - 1)
        s = s + roll(mid, -1, 0) + roll(mid, 1, 0)
        s = s + roll(mid, -1, 1) + roll(mid, 1, 1)
        return mid, s

    def defect_of(mid, s, f, k):
        return f - (d[k] * mid - w[k] * s)

    def beside0(i):
        lane = lanes((32, 128))
        mid = [VM[i, 0:32], VH[i, 0:32]]
        up = [roll(m, -1, 1) for m in mid]
        down = [roll(m, 1, 1) for m in mid]
        sums = []
        for k, ref in enumerate((VM, VH)):
            s = ref[i + 1, 0:32] + ref[i - 1, 0:32]
            s = s + roll(mid[k], -1, 0) + roll(mid[k], 1, 0)
            s = s + jnp.where(lane == 127, up[1 - k], up[k]) + jnp.where(lane == 0, down[1 - k], down[k])
            sums.append(s)
        return mid, sums

    inputs[0].wait()
    loads[0].wait()
    rows = []
    for x in range(8):
        s = None
        for a in range(2):
            for b in range(2):
                part = src[2 * x + a, pl.ds(b, 8, stride=2), :]
                s = part if s is None else s + part
        rows.append(s)
    f1o[0:8] = mm2(jnp.concatenate(rows, axis=0), mats[RZ1]).reshape(8, 8, 128)
    restrict12(f1o, 0)
    inputs[1].wait()
    shift = shift_ref[0]
    w = [0.25**k for k in range(4)]
    d = [6.0 * w[k] + shift for k in range(3)]
    c = [jnp.max(DAMPING / jnp.full((8, 128), d[k], jnp.float32)) for k in range(3)]

    ends = mm2(src[...].reshape(256, 128), mats[PACK]).reshape(16, 2, 8, 128)
    spot = lax.div(lanes((16, 8, 128)), 16) == lax.broadcasted_iota(jnp.int32, (16, 8, 128), 1)
    for y in range(2):
        PK[y] = jnp.sum(jnp.where(spot, ends[:, y], 0.0), axis=1)
    pl.semaphore_wait(barrier, len(friends))
    pending = []
    first = gather_first(0)
    pending += first
    side = []
    for dy, k in ((1, 0), (3, 1)):
        side.append(remote(f1o.at[pl.ds(0, 8)], LR1.at[k], peer(0, dy, 0)))
    for dy, k in ((1, 0), (3, 1)):
        side.append(remote(PK, LR0.at[k], peer(0, dy, 0)))
    for copy in side:
        copy.start()
    pending += side

    second = gather_second(0, first)
    pending += second.values()

    side[0].wait_recv()
    side[1].wait_recv()
    lane = lanes((8, 8, 128))
    F1[8:16, 8:16] = jnp.where(
        lane < 8,
        roll(LR1[0], 64, 2),
        jnp.where(lane < 72, f1o[0:8], jnp.where(lane < 80, roll(LR1[1], 64, 2), 0.0)),
    )
    corner1 = []
    around = [(1, 0), (-1, 0), (0, 1), (0, -1), (1, 1), (1, -1), (-1, 1), (-1, -1)]
    for dx, dz in around:
        (n_x, from_x, to_x), (n_y, from_y, to_y) = (
            {0: (8, 8, 8), 1: (6, 10, 2), -1: (6, 8, 16)}[step] for step in (dx, dz)
        )
        corner1.append(
            remote(
                F1.at[pl.ds(from_x, n_x), pl.ds(from_y, n_y)],
                F1.at[pl.ds(to_x, n_x), pl.ds(to_y, n_y)],
                peer(dx, 0, dz),
            )
        )
    for copy in corner1:
        copy.start()
    pending += corner1

    side[2].wait_recv()
    side[3].wait_recv()

    after = lax.rem(lanes((2, 16, 128)), 16) < 8
    HP[1:3, 6:22] = jnp.where(after, LR0[1], LR0[0])
    F0M[6:22, 8:24] = src[...]

    third = gather_third(0, second)
    pending += third

    corner0, packed0 = [], []
    for dx, dz in around:
        n_x, from_x, to_x = {0: (16, 0, 6), 1: (5, 11, 1), -1: (5, 0, 22)}[dx]
        n_y, from_y, to_y = {0: (16, 0, 8), 1: (6, 10, 2), -1: (6, 0, 24)}[dz]
        corner0.append(
            remote(
                src.at[pl.ds(from_x, n_x), pl.ds(from_y, n_y)],
                F0M.at[pl.ds(to_x, n_x), pl.ds(to_y, n_y)],
                peer(dx, 0, dz),
            )
        )
        n_g, from_g, to_g = {0: (2, 1, 1), 1: (1, 2, 0), -1: (1, 1, 3)}[dz]
        packed0.append(
            remote(
                HP.at[pl.ds(from_g, n_g), pl.ds(from_x + 6, n_x)],
                HP.at[pl.ds(to_g, n_g), pl.ds(to_x, n_x)],
                peer(dx, 0, dz),
            )
        )
    for copy in packed0 + corner0:
        copy.start()
    pending += packed0 + corner0

    unpack(0)
    loads[1].wait()
    loads[2].wait()

    def sum3(t):
        keep3([G2[j, pl.ds(4 * t + 1, 4)] for j in range(4)], t)

    loop(0, 8, sum3, 2)
    u = solve3(WQ, CUBIC, 0, 32)
    for j in range(4):
        U2[j, 1:33] = u[j]
    wrap(U2)
    sweep2(U2, V2, 0, 32)
    wrap(V2)
    defect2()
    correct2(False)

    refine21_z(QZ21)
    refine21(CUBIC, 3, 9)
    for copy in corner1:
        copy.wait_recv()

    def pre1(i):
        mid, s = beside1(lambda k: B1[k, 0:24], i)
        V1[i] = mid + c[1] * defect_of(mid, s, F1[i], 1)

    loop(7, 17, pre1, 10)

    def res1(i):
        mid, s = beside1(lambda k: V1[k], i)
        T1[i - 8] = defect_of(mid, s, F1[i], 1)

    loop(8, 16, res1, 8)
    restrict12(T1, 8)
    first = gather_first(1)
    second = gather_second(1, first)
    refine21(CUBIC, 0, 3)
    refine21(CUBIC, 9, 12)
    loop(2, 7, pre1, 5)
    loop(17, 22, pre1, 5)
    for copy in packed0:
        copy.wait_recv()

    def open0(i):
        spot = lax.div(lanes((4, 8, 128)), 16) == lax.broadcasted_iota(jnp.int32, (4, 8, 128), 1)
        rows = jnp.where(spot, jnp.broadcast_to(HP[:, i].reshape(4, 1, 128), (4, 8, 128)), 0.0)
        BH[i, 0:32] = rows.reshape(32, 128)

    loop(1, 27, open0, 2)
    F0H[1:27, 0:32] = mm2(BH[1:27, 0:32].reshape(832, 128), mats[OPEN]).reshape(26, 32, 128)
    third = gather_third(1, second)
    pending += first + list(second.values()) + third
    unpack(1)
    cycle2_zero()
    refine21_z(PZ21)
    refine21(LINEAR, 0, 12)

    def add1(i):
        V1[i] = V1[i] + B1[i, 0:24]

    loop(2, 22, add1, 4)

    def post1(i):
        mid, s = beside1(lambda k: V1[k], i)
        U1[i - 3] = mid + c[1] * defect_of(mid, s, F1[i], 1)

    loop(3, 21, post1, 9)

    u = U1[...].reshape(432, 128)
    TZM[...] = mm2(u, mats[QZ10M]).reshape(18, 24, 128)
    TZH[...] = mm2(u, mats[QZ10H]).reshape(18, 24, 128)

    def cubic0(t):
        for source, target in ((TZM, BM), (TZH, BH)):
            for p in range(2):
                plane = weighted(CUBIC[p], lambda off: source[t + 2 + off])
                at = {off: roll(plane, -(4 + off), 0)[0:16] for off in range(-2, 3)}
                for q in range(2):
                    target[2 * t + p, pl.ds(q, 16, stride=2), :] = weighted(CUBIC[q], at.__getitem__)

    loop(1, 13, cubic0, 6)
    for copy in corner0:
        copy.wait_recv()

    def pre0(i):
        lane = lanes((32, 128))
        refs = (BM, BH)
        mid = [ref[i, 0:32] for ref in refs]
        up = [roll(m, -1, 1) for m in mid]
        down = [roll(m, 1, 1) for m in mid]
        for k, (f, v) in enumerate(((F0M, VM), (F0H, VH))):
            s = refs[k][i + 1, 0:32] + refs[k][i - 1, 0:32]
            s = s + roll(mid[k], -1, 0) + roll(mid[k], 1, 0)
            s = s + jnp.where(lane == 127, up[1 - k], up[k]) + jnp.where(lane == 0, down[1 - k], down[k])
            v[i, 0:32] = mid[k] + c[0] * defect_of(mid[k], s, f[i, 0:32], 0)

    loop(3, 25, pre0, 22)

    def res0(t):
        for a in range(2):
            i = 2 * t + 2 + a
            mid, sums = beside0(i)
            for k, (f, target) in enumerate(((F0M, TM), (F0H, TH))):
                r = defect_of(mid[k], sums[k], f[i, 0:32], 0)
                target[t, 0:32] = r if a == 0 else target[t, 0:32] + r
        for source, target in ((TM, RM), (TH, RHH)):
            target[t, 0:16] = source[t, pl.ds(0, 16, stride=2), :] + source[t, pl.ds(1, 16, stride=2), :]

    loop(1, 11, res0, 10)
    R1[1:11, 0:16] = (
        mm2(RM[1:11, 0:16].reshape(160, 128), mats[RZ1]) + mm2(RHH[1:11, 0:16].reshape(160, 128), mats[RH])
    ).reshape(10, 16, 128)

    def zero1(i):
        D1[i, 0:16] = c[1] * R1[i, 0:16]

    loop(1, 11, zero1, 5)

    def res1b(i):
        mid, s = beside1(lambda k: D1[k, 0:16], i)
        T1[i - 2, 0:16] = defect_of(mid, s, R1[i, 0:16], 1)

    loop(2, 10, res1b, 8)
    restrict12(T1, 4)
    first = gather_first(2)
    second = gather_second(2, first)
    for t in (0, 13):
        cubic0(t)
    for i in (1, 2, 25, 26):
        pre0(i)
    for t in (0, 11):
        res0(t)
        R1[t, 0:16] = mm2(RM[t, 0:16], mats[RZ1]) + mm2(RHH[t, 0:16], mats[RH])
        zero1(t)
    third = gather_third(2, second)
    pending += first + list(second.values()) + third
    unpack(2)
    cycle2_zero()
    refine21_z(PZ21)
    refine21(LINEAR, 3, 9)

    def add1b(i):
        D1[i, 0:16] = D1[i, 0:16] + B1[i + 6, 4:20]

    loop(0, 12, add1b, 4)
    E1[0, 0:16] = jnp.zeros((16, 128), jnp.float32)
    E1[11, 0:16] = jnp.zeros((16, 128), jnp.float32)

    def post1b(i):
        mid, s = beside1(lambda k: D1[k, 0:16], i)
        E1[i, 0:16] = mid + c[1] * defect_of(mid, s, R1[i, 0:16], 1)

    loop(1, 11, post1b, 10)

    e = E1[:, 0:16].reshape(192, 128)
    TZM[0:12, 0:16] = mm2(e, mats[PZ10M]).reshape(12, 16, 128)
    TZH[0:12, 0:16] = mm2(e, mats[PZ10H]).reshape(12, 16, 128)

    def linear0(t):
        for source, target, v in ((TZM, BM, VM), (TZH, BH, VH)):
            for p in range(2):
                plane = weighted(LINEAR[p], lambda off: source[t + 1 + off, 0:16])
                i = 2 * t + 4 + p
                for q in range(2):
                    target[i, pl.ds(q, 16, stride=2), :] = weighted(LINEAR[q], lambda off: roll(plane, -off, 0))
                v[i, 0:32] = v[i, 0:32] + target[i, 0:32]

    loop(0, 10, linear0, 5)

    def post0(i):
        mid, sums = beside0(i)
        v = mid[0] + c[0] * defect_of(mid[0], sums[0], F0M[i, 0:32], 0)
        out[i - 6] = v[8:24]

    loop(6, 22, post0, 16)
    for copy in pending:
        copy.wait_send()


def solution(mesh):
    mats, hxy, lam = tables()
    f32 = jnp.float32
    vmem = pltpu.VMEM
    scratch = [
        pltpu.SMEM((1,), f32),
        vmem((16, 16, 128), f32),
        vmem((17, 128, 128), jnp.bfloat16),
        vmem((4, 256, 256), jnp.bfloat16),
        vmem((256, 128), f32),
        vmem((3, 32, 128), f32),
        vmem((3, 4, 8 * SLOT, 128), f32),
        vmem((10, 8, 128), f32),
        vmem((2, 8, 8, 128), f32),
        vmem((2, 2, 16, 128), f32),
        vmem((2, 16, 128), f32),
        vmem((4, 40, 128), f32),
        vmem((24, 24, 128), f32),
        vmem((28, 40, 128), f32),
        vmem((28, 40, 128), f32),
        vmem((4, 34, 8, 128), f32),
        vmem((4, 34, 8, 128), f32),
        vmem((4, 34, 8, 128), f32),
        vmem((2, 16, 8, 128), f32),
        vmem((4, 16, 8, 128), f32),
        vmem((26, 40, 128), f32),
        vmem((24, 24, 128), f32),
        vmem((18, 24, 128), f32),
        vmem((9, 24, 128), f32),
        vmem((48, 128), f32),
        vmem((18, 24, 128), f32),
        vmem((18, 24, 128), f32),
        vmem((28, 40, 128), f32),
        vmem((28, 40, 128), f32),
        vmem((28, 40, 128), f32),
        vmem((28, 40, 128), f32),
        vmem((12, 40, 128), f32),
        vmem((12, 40, 128), f32),
        vmem((12, 24, 128), f32),
        vmem((12, 24, 128), f32),
        vmem((12, 24, 128), f32),
        vmem((12, 24, 128), f32),
        vmem((12, 24, 128), f32),
        pltpu.SemaphoreType.DMA((5,)),
        pltpu.SemaphoreType.DMA((N_SEMS,)),
        pltpu.SemaphoreType.DMA((N_SEMS,)),
    ]

    def step(source, shift):
        return pl.pallas_call(
            kernel,
            out_shape=jax.ShapeDtypeStruct(source.shape, f32),
            in_specs=[
                pl.BlockSpec(memory_space=pl.ANY),
            ]
            * 5,
            out_specs=pl.BlockSpec(memory_space=vmem),
            scratch_shapes=scratch,
            compiler_params=pltpu.CompilerParams(collective_id=0, has_side_effects=True),
            name="fcycle",
        )(shift, source, jnp.asarray(mats), jnp.asarray(hxy), jnp.asarray(lam))

    spec = P("gx", "gz", "gy")
    return jax.shard_map(step, mesh=mesh, in_specs=(spec, P()), out_specs=spec, check_vma=False)
```
